32 devices in a mesh: outer: 4 (over y, core), inner: 8 (over z, x).
Axes of the slice: x: 2, y: 2, z: 4, core: 2. Of those that a mesh axis runs over, the one named last changes fastest.
Arguments:
- amplitudes: float32 [2, 8388608], P(None, ('outer', 'inner')), may hold values from -200 to 200
Outputs:
- transformed: float32 [2, 8388608], P(None, ('outer', 'inner'))
- checks: float32 [3], replicated
The draws below stay inside these ranges and needn't reach their ends.
All inputs are finite; a program needn't handle non-finite values.
Results may differ from the reference program's by a relative error of at most 0.00007.
Values sent between devices are 32-bit elements; how exact they have to be, the bound alone decides.
No kernel may reach another device: no remote copies, remote signals or barrier semaphores. Data moves between devices by JAX's collectives and lax.ppermute only.
A program may use at most 64 MiB of HBM per device.

```python
import math
import jax
import jax.numpy as jnp
from jax import lax

AMP_DEV = 262144
WINDOW = 9
DEVICES = 32


def draw_amplitudes(key, part):
    total_len = AMP_DEV * DEVICES
    first, second = jax.random.split(key, 2)
    position = jnp.arange(total_len, dtype=jnp.int32)
    device_pos = (position // AMP_DEV).astype(jnp.float32) / max(DEVICES - 1, 1)
    cell_scale = jnp.exp(jax.random.uniform(second, (total_len,), jnp.float32) * math.log(10.0))
    values = jnp.clip(jax.random.normal(first, (2, total_len), jnp.float32), -5.0, 5.0)
    ramp = 3.0 ** device_pos
    return values * ramp * cell_scale / 3.0


def setup_inputs(seed: int = 0) -> dict:
    streams_of = jax.random.split(jax.random.key(seed), 2)
    return {
        "amplitudes": draw_amplitudes(jax.random.fold_in(streams_of[1], 71), 0),
    }


def bit_reverse_table(count):
    result = []
    for value in range(2 ** count):
        flipped = 0
        for bit_pos in range(count):
            flipped = flipped | (value >> bit_pos & 1) << count - 1 - bit_pos
        result.append(flipped)
    return jnp.array(result, dtype=jnp.int32)

def reference(amplitudes):
    columns = 2 ** WINDOW
    total_len = AMP_DEV * DEVICES
    qubits = total_len.bit_length() - 1
    complex_amp = lax.complex(amplitudes[0], amplitudes[1]).reshape(-1, columns)
    spectrum = jnp.fft.ifft(complex_amp, axis=-1) * math.sqrt(columns)
    windowed = spectrum[:, bit_reverse_table(WINDOW)].reshape(-1)
    stacked = jnp.stack([jnp.real(windowed), jnp.imag(windowed)])
    expanded = stacked.reshape((2,) + (2,) * qubits)
    reversed_field = jnp.transpose(expanded, [0] + list(range(qubits, 0, -1))).reshape(2, total_len)
    mean_square = jnp.sum(reversed_field * reversed_field) / total_len
    factor = lax.rsqrt(mean_square + 1e-06)
    transformed = reversed_field * factor
    angles = jnp.arange(total_len, dtype=jnp.int32).astype(jnp.float32) * (2.0 * math.pi / total_len)
    cosine = jnp.cos(angles)
    sine = jnp.sin(angles)
    scaled = 1.0 / math.sqrt(total_len)
    phase_real = jnp.sum(transformed[0] * cosine + transformed[1] * sine) * scaled
    phase_imag = jnp.sum(transformed[1] * cosine - transformed[0] * sine) * scaled
    return (transformed, jnp.stack([mean_square, phase_real, phase_imag]))
```

```python
import math

import jax
import jax.numpy as jnp
import ml_dtypes
import numpy as np
from jax import lax
from jax.experimental import pallas as pl
from jax.experimental.pallas import tpu as pltpu
from jax.sharding import PartitionSpec as P

WINDOW = 9
LANES = 128
RADIX = 2**WINDOW // LANES
AXES = ("outer", "inner")


def flip(value, count):
    result = 0
    for bit_pos in range(count):
        result |= (value >> bit_pos & 1) << count - 1 - bit_pos
    return result


def split_halves(table):
    high = table.astype(ml_dtypes.bfloat16)
    low = (table - high.astype(np.float64)).astype(ml_dtypes.bfloat16)
    return high, low


def transform_tables():
    columns = 2**WINDOW
    freq = np.arange(LANES) * RADIX
    sample = np.arange(LANES)
    tables = []
    for residue in range(RADIX):
        angles = (freq + residue)[:, None] * sample[None, :] % columns * (2 * np.pi / columns)
        cosine = np.cos(angles) / math.sqrt(columns)
        sine = np.sin(angles) / math.sqrt(columns)
        rows = np.stack([np.concatenate([cosine, -sine], 1), np.concatenate([sine, cosine], 1)], 1)
        tables.append(rows.reshape(2 * LANES, 2 * LANES))
    return split_halves(np.stack(tables))


def halves(values):
    high = values.astype(jnp.bfloat16)
    low = (values - high.astype(jnp.float32)).astype(jnp.bfloat16)
    return high, low


def dot_rows(left, right):
    return lax.dot_general(
        left, right, (((1,), (1,)), ((), ())), preferred_element_type=jnp.float32
    )


def transform_kernel(
    info, x_ref, high_ref, low_ref, order_ref, send_ref, stage, square_sum, real_sum, imag_sum, sems
):
    n_devices, chunks, angle_scale, device_id = info()
    chunk = pl.program_id(0)
    chunk_rows = RADIX * 8

    @pl.when(chunk == 0)
    def _():
        square_sum[...] = jnp.zeros_like(square_sum)
        real_sum[...] = jnp.zeros_like(real_sum)
        imag_sum[...] = jnp.zeros_like(imag_sum)

    parts = [
        [x_ref[pl.ds(2 * j + s, LANES, stride=2 * RADIX), :] for s in range(2)]
        for j in range(RADIX)
    ]
    squares = sum(p * p for pair in parts for p in pair)
    square_sum[...] += squares.reshape(LANES // 8, 8, LANES).sum(0)

    dev_bits = n_devices.bit_length() - 1
    chunk_bits = chunks.bit_length() - 1
    base = jnp.int32(0)
    for bit in range(dev_bits):
        base += (device_id >> bit & 1) << (dev_bits - 1 - bit)
    for bit in range(chunk_bits):
        base += (chunk >> bit & 1) << (dev_bits + chunk_bits - 1 - bit)
    theta = (order_ref[...] * float(n_devices * chunks) + base.astype(jnp.float32)) * angle_scale
    lane = lax.broadcasted_iota(jnp.int32, (LANES, LANES), 1)
    theta_sq = theta * theta
    cosine = 1.0 - theta_sq * (0.5 - theta_sq * (1.0 / 24.0))
    sine = theta * (1.0 - theta_sq * (1.0 / 6.0 - theta_sq * (1.0 / 120.0)))
    cosine = jnp.where(lane == 1, cosine, 0.0)
    sine = jnp.where(lane == 1, sine, 0.0)
    first_re, first_im = parts[0]
    real_terms = first_re * cosine + first_im * sine
    imag_terms = first_im * cosine - first_re * sine
    real_sum[...] += real_terms.reshape(LANES // 8, 8, LANES).sum(0)
    imag_sum[...] += imag_terms.reshape(LANES // 8, 8, LANES).sum(0)

    (r0, i0), (r1, i1), (r2, i2), (r3, i3) = parts
    ar, ai, br, bi = r0 + r2, i0 + i2, r0 - r2, i0 - i2
    cr, ci, dr, di = r1 + r3, i1 + i3, r1 - r3, i1 - i3
    folded = [(ar + cr, ai + ci), (br - di, bi + dr), (ar - cr, ai - ci), (br + di, bi - dr)]
    for residue in range(RADIX):
        high, low = halves(jnp.concatenate(folded[residue], 1))
        table = high_ref[residue]
        values = dot_rows(table, high) + dot_rows(table, low) + dot_rows(low_ref[residue], high)
        row = pl.multiple_of(chunk * chunk_rows + residue * 8, 8)
        stage[:, pl.ds(row, 8), :] = values.reshape(n_devices, 8, LANES)

    def send(step):
        rows = pl.ds(pl.multiple_of(step * chunk_rows, 8), chunk_rows)
        return pltpu.make_async_copy(stage.at[:, rows], send_ref.at[:, rows], sems.at[step])

    send(chunk).start()

    @pl.when(chunk == chunks - 1)
    def _():
        rows = pl.ds(chunks * chunk_rows, 8)
        sums = [ref[...].sum(0, keepdims=True) for ref in (square_sum, real_sum, imag_sum)]
        tile = jnp.concatenate(sums + [jnp.zeros((5, LANES), jnp.float32)], 0)
        stage[:, rows, :] = jnp.broadcast_to(tile[None], (n_devices, 8, LANES))
        last = pltpu.make_async_copy(stage.at[:, rows], send_ref.at[:, rows], sems.at[chunks])
        last.start()
        for step in range(chunks):
            send(step).wait()
        last.wait()


def place_kernel(info, recv_ref, order_ref, out_ref, checks_ref, held, factor_ref, sems):
    n_devices, chunks, total_len = info
    group = pl.program_id(0)
    dev_bits = n_devices.bit_length() - 1
    chunk_bits = chunks.bit_length() - 1
    slot_rows = held.shape[0] // n_devices

    @pl.when(group == 0)
    def _():
        copies = [
            pltpu.make_async_copy(
                recv_ref.at[source],
                held.at[pl.ds(flip(source, dev_bits) * slot_rows, slot_rows)],
                sems.at[source],
            )
            for source in range(n_devices)
        ]
        for copy in copies:
            copy.start()
        for copy in copies:
            copy.wait()
        tile = held[pl.ds(slot_rows - 8, 8), :]
        for source in range(1, n_devices):
            tile = tile + held[pl.ds(source * slot_rows + slot_rows - 8, 8), :]
        sums = tile.sum(1, keepdims=True)
        mean_square = jnp.broadcast_to(sums[0:1], (8, LANES)) * (1.0 / total_len)
        shifted = mean_square + 1e-06
        factor = lax.rsqrt(shifted)
        factor = factor * (1.5 - 0.5 * shifted * factor * factor)
        factor_ref[...] = factor
        columns = 2**WINDOW
        scaled = factor * math.sqrt(columns / total_len)
        checks_ref[0] = mean_square[0, 0]
        checks_ref[1] = (jnp.broadcast_to(sums[1:2], (8, LANES)) * scaled)[0, 0]
        checks_ref[2] = (jnp.broadcast_to(sums[2:3], (8, LANES)) * scaled)[0, 0]

    factor = jnp.broadcast_to(factor_ref[0:1], (LANES, LANES))
    order = order_ref[...]
    for residue in range(RADIX):
        for part in range(2):
            pieces = []
            for low in range(chunks):
                tile_row = (flip(low, chunk_bits) * RADIX + residue) * 8 + part
                pieces.append(held[pl.ds(tile_row + 2 * group, n_devices, stride=slot_rows), :])
            high, low = halves(jnp.concatenate(pieces, 0))
            turned = dot_rows(order, jnp.concatenate([high, low], 1))
            out_ref[pl.ds(residue * 2 * LANES + part, LANES, stride=2), :] = turned * factor


def reverse_index(values, count):
    result = jnp.zeros_like(values)
    for bit_pos in range(count):
        result = result | (values >> bit_pos & 1) << count - 1 - bit_pos
    return result


def reversal_table(size, count):
    indices = jnp.arange(size, dtype=jnp.int32)
    return (reverse_index(indices, count)[:, None] == indices[None, :]).astype(jnp.float32)


def check_terms(current, positions, angle_scale):
    angles = positions.astype(jnp.float32) * angle_scale
    cosine = jnp.cos(angles)
    sine = jnp.sin(angles)
    squares = jnp.sum(current * current)
    phase_real = jnp.sum(current[0] * cosine + current[1] * sine)
    phase_imag = jnp.sum(current[1] * cosine - current[0] * sine)
    return (squares, phase_real, phase_imag)


def general_device(amplitudes):
    amp_dev = amplitudes.shape[1]
    n_outer = lax.axis_size("outer")
    n_inner = lax.axis_size("inner")
    outer_bits = n_outer.bit_length() - 1
    inner_bits = n_inner.bit_length() - 1
    global_bits = outer_bits + inner_bits
    local_bits = amp_dev.bit_length() - 1
    n_devices = n_outer * n_inner
    high_count = amp_dev // n_devices
    total_len = amp_dev * n_devices
    columns = 2**WINDOW
    rows_count = amp_dev // columns
    column_ids = jnp.arange(columns, dtype=jnp.int32)
    reversed_ids = reverse_index(column_ids, WINDOW)
    products = column_ids[:, None] * reversed_ids[None, :] % columns
    angles = products.astype(jnp.float32) * (2.0 * math.pi / columns)
    real_part = jnp.cos(angles) / math.sqrt(columns)
    imag_part = jnp.sin(angles) / math.sqrt(columns)
    table = jnp.concatenate(
        [jnp.concatenate([real_part, imag_part], 1), jnp.concatenate([-imag_part, real_part], 1)], 0
    )
    stacked = jnp.concatenate(
        [amplitudes[0].reshape(rows_count, columns), amplitudes[1].reshape(rows_count, columns)], 1
    )
    result = jnp.dot(
        stacked, table, precision=lax.Precision.HIGHEST, preferred_element_type=jnp.float32
    )
    windowed = jnp.stack([result[:, :columns].reshape(-1), result[:, columns:].reshape(-1)])
    device_id = lax.axis_index("outer") * n_inner + lax.axis_index("inner")
    angle_scale = 2.0 * math.pi / total_len
    local_ids = jnp.arange(amp_dev, dtype=jnp.int32)
    positions = reverse_index(device_id * amp_dev + local_ids, local_bits + global_bits)
    totals = lax.psum(check_terms(windowed, positions, angle_scale), ("outer", "inner"))
    device_table = reversal_table(n_devices, global_bits)
    high_table = reversal_table(high_count, local_bits - global_bits)
    grid = windowed.reshape(2, high_count, n_devices)
    ordered = jnp.einsum("pm,shm->sph", device_table, grid, precision=lax.Precision.HIGHEST)
    blocks = ordered.reshape(2, n_outer, n_inner, high_count)
    blocks = lax.all_to_all(
        lax.all_to_all(blocks, "outer", split_axis=1, concat_axis=1, tiled=True),
        "inner",
        split_axis=2,
        concat_axis=2,
        tiled=True,
    )
    received = blocks.reshape(2, n_devices, high_count)
    turned_high = jnp.einsum("qh,sdh->sdq", high_table, received, precision=lax.Precision.HIGHEST)
    placed = jnp.einsum("ed,sdq->sqe", device_table, turned_high, precision=lax.Precision.HIGHEST)
    reversed_field = placed.reshape(2, amp_dev)
    mean_square = totals[0] / total_len
    factor = lax.rsqrt(mean_square + 1e-06)
    scaled = factor / math.sqrt(total_len)
    checks = jnp.stack([mean_square, totals[1] * scaled, totals[2] * scaled])
    return (reversed_field * factor, checks)


def per_device(amplitudes):
    amp_dev = amplitudes.shape[1]
    n_devices = lax.axis_size("outer") * lax.axis_size("inner")
    n_inner = lax.axis_size("inner")
    total_len = amp_dev * n_devices
    columns = 2**WINDOW
    rows_count = amp_dev // columns
    chunks = rows_count // LANES
    groups = columns // n_devices // RADIX
    if chunks * n_devices != LANES or groups * 2 != 8:
        return general_device(amplitudes)
    vectors = 2 * amp_dev // LANES
    slot_rows = chunks * RADIX * 8 + 8
    x = amplitudes.reshape(2, vectors // 2, LANES).transpose(1, 0, 2).reshape(vectors, LANES)
    high, low = transform_tables()
    turn = np.array([flip(lane, LANES.bit_length() - 1) for lane in range(LANES)])
    order = (turn[:, None] == np.arange(LANES)[None, :]).astype(np.float32)
    order = np.concatenate([order, order], 1).astype(ml_dtypes.bfloat16)
    turn_table = np.broadcast_to(turn[:, None], (LANES, LANES)).astype(np.float32)

    def info():
        device_id = lax.axis_index("outer") * n_inner + lax.axis_index("inner")
        return n_devices, chunks, 2.0 * math.pi / total_len, device_id

    whole = lambda shape: pl.BlockSpec(shape, lambda i: (0,) * len(shape))
    sent = pl.pallas_call(
        lambda *refs: transform_kernel(info, *refs),
        grid=(chunks,),
        in_specs=[
            pl.BlockSpec((vectors // chunks, LANES), lambda i: (i, 0)),
            whole(high.shape),
            whole(low.shape),
            whole(turn_table.shape),
        ],
        out_specs=pl.BlockSpec(memory_space=pltpu.HBM),
        out_shape=jax.ShapeDtypeStruct((n_devices, slot_rows, LANES), jnp.float32),
        scratch_shapes=[
            pltpu.VMEM((n_devices, slot_rows, LANES), jnp.float32),
            pltpu.VMEM((8, LANES), jnp.float32),
            pltpu.VMEM((8, LANES), jnp.float32),
            pltpu.VMEM((8, LANES), jnp.float32),
            pltpu.SemaphoreType.DMA((chunks + 1,)),
        ],
        name="transform",
    )(x, jnp.asarray(high), jnp.asarray(low), jnp.asarray(turn_table))
    received = lax.all_to_all(sent, AXES, 0, 0, tiled=True)
    placed, checks = pl.pallas_call(
        lambda *refs: place_kernel((n_devices, chunks, total_len), *refs),
        grid=(groups,),
        in_specs=[pl.BlockSpec(memory_space=pltpu.HBM), whole(order.shape)],
        out_specs=[
            pl.BlockSpec((vectors // groups, LANES), lambda i: (i, 0)),
            pl.BlockSpec(memory_space=pltpu.SMEM),
        ],
        out_shape=[
            jax.ShapeDtypeStruct((vectors, LANES), jnp.float32),
            jax.ShapeDtypeStruct((3,), jnp.float32),
        ],
        scratch_shapes=[
            pltpu.VMEM((n_devices * slot_rows, LANES), jnp.float32),
            pltpu.VMEM((8, LANES), jnp.float32),
            pltpu.SemaphoreType.DMA((n_devices,)),
        ],
        name="place",
    )(received, jnp.asarray(order))
    placed = placed.reshape(vectors // 2, 2, LANES).transpose(1, 0, 2).reshape(2, amp_dev)
    return placed, checks


def solution(mesh):
    return jax.shard_map(
        per_device,
        mesh=mesh,
        in_specs=(P(None, ("outer", "inner")),),
        out_specs=(P(None, ("outer", "inner")), P()),
        check_vma=False,
    )
```

```python
import math

import jax
import jax.numpy as jnp
import ml_dtypes
import numpy as np
from jax import lax
from jax.experimental import pallas as pl
from jax.experimental.pallas import tpu as pltpu
from jax.sharding import PartitionSpec as P


WINDOW = 9
LANES = 128
RADIX = 2**WINDOW // LANES
AXES = ("outer", "inner")
VMEM_LIMIT = 16 * 2**20


def flip(value, count):
    result = 0
    for bit_pos in range(count):
        result |= (value >> bit_pos & 1) << count - 1 - bit_pos
    return result


def split_halves(table):
    high = table.astype(ml_dtypes.bfloat16)
    low = (table - high.astype(np.float64)).astype(ml_dtypes.bfloat16)
    return high, low


def transform_tables():
    columns = 2**WINDOW
    freq = np.arange(LANES) * RADIX
    sample = np.arange(LANES)
    tables = []
    for residue in range(RADIX):
        angles = (freq + residue)[:, None] * sample[None, :] % columns * (2 * np.pi / columns)
        cosine = np.cos(angles) / math.sqrt(columns)
        sine = np.sin(angles) / math.sqrt(columns)
        rows = np.stack([np.concatenate([cosine, -sine], 1), np.concatenate([sine, cosine], 1)], 1)
        tables.append(rows.reshape(2 * LANES, 2 * LANES))
    return split_halves(np.stack(tables))


def halves(values):
    high = values.astype(jnp.bfloat16)
    low = (values - high.astype(jnp.float32)).astype(jnp.bfloat16)
    return high, low


def dot_rows(left, right):
    return lax.dot_general(
        left, right, (((1,), (1,)), ((), ())), preferred_element_type=jnp.float32
    )


def transform_kernel(info, targets, tiles, x_hbm, high_hbm, low_hbm, order_hbm, *refs):
    n_devices, chunks, angle_scale, device_id = info()
    outs, (x_ref, high_ref, low_ref, order_ref, stage, sems) = refs[:-6], refs[-6:]
    chunk_rows = RADIX * 8
    x_rows = x_ref.shape[0] // chunks
    dev_bits = n_devices.bit_length() - 1
    chunk_bits = chunks.bit_length() - 1

    def load(source, target, index):
        return pltpu.make_async_copy(source, target, sems.at[index])

    loads = []
    for chunk in range(chunks):
        rows = pl.ds(chunk * x_rows, x_rows)
        loads.append(load(x_hbm.at[rows], x_ref.at[rows], chunk))
    sides = [load(order_hbm, order_ref, chunks)]
    tables = []
    for residue in range(RADIX):
        index = chunks + 1 + 2 * residue
        tables.append(
            [
                load(high_hbm.at[residue], high_ref.at[residue], index),
                load(low_hbm.at[residue], low_ref.at[residue], index + 1),
            ]
        )
    for copy in loads[:1] + sides + sum(tables, []) + loads[1:]:
        copy.start()

    base = jnp.int32(0)
    for bit in range(dev_bits):
        base += (device_id >> bit & 1) << (dev_bits - 1 - bit)
    lane = lax.broadcasted_iota(jnp.int32, (LANES, LANES), 1)
    square_sum = real_sum = imag_sum = jnp.zeros((8, LANES), jnp.float32)
    for chunk in range(chunks):
        loads[chunk].wait()
        parts = [
            [
                x_ref[pl.ds(chunk * x_rows + 2 * j + s, LANES, stride=2 * RADIX), :]
                for s in range(2)
            ]
            for j in range(RADIX)
        ]
        squares = sum(p * p for pair in parts for p in pair)
        square_sum += squares.reshape(LANES // 8, 8, LANES).sum(0)

        if chunk == 0:
            sides[0].wait()
        offset = (base + n_devices * flip(chunk, chunk_bits)).astype(jnp.float32)
        theta = (order_ref[...] * float(n_devices * chunks) + offset) * angle_scale
        theta_sq = theta * theta
        cosine = 1.0 - theta_sq * (0.5 - theta_sq * (1.0 / 24.0))
        sine = theta * (1.0 - theta_sq * (1.0 / 6.0 - theta_sq * (1.0 / 120.0)))
        cosine = jnp.where(lane == 1, cosine, 0.0)
        sine = jnp.where(lane == 1, sine, 0.0)
        first_re, first_im = parts[0]
        real_terms = first_re * cosine + first_im * sine
        imag_terms = first_im * cosine - first_re * sine
        real_sum += real_terms.reshape(LANES // 8, 8, LANES).sum(0)
        imag_sum += imag_terms.reshape(LANES // 8, 8, LANES).sum(0)

        (r0, i0), (r1, i1), (r2, i2), (r3, i3) = parts
        ar, ai, br, bi = r0 + r2, i0 + i2, r0 - r2, i0 - i2
        cr, ci, dr, di = r1 + r3, i1 + i3, r1 - r3, i1 - i3
        folded = [(ar + cr, ai + ci), (br - di, bi + dr), (ar - cr, ai - ci), (br + di, bi - dr)]
        for residue in range(RADIX):
            high, low = halves(jnp.concatenate(folded[residue], 1))
            if chunk == 0:
                for copy in tables[residue]:
                    copy.wait()
            table = high_ref[residue]
            values = dot_rows(table, high) + dot_rows(table, low) + dot_rows(low_ref[residue], high)
            stage[:, residue * 8 : residue * 8 + 8, :] = values.reshape(n_devices, 8, LANES)
        for mask, out, row in targets:
            rows = pl.ds(row + chunk * chunk_rows, chunk_rows)
            outs[out][rows, :] = stage[device_id ^ mask]

    sums = [value.sum(0, keepdims=True) for value in (square_sum, real_sum, imag_sum)]
    tile = jnp.concatenate(sums + [jnp.zeros((5, LANES), jnp.float32)], 0)
    for out, row in tiles:
        outs[out][pl.ds(row, 8), :] = tile


def join_kernel(plan, n_join, swapped_ref, own_ref, *refs):
    outs = refs[n_join:]
    rows, tile_row = plan
    tile = swapped_ref[pl.ds(tile_row, 8), :] + own_ref[pl.ds(rows, 8), :]
    for index in range(n_join):
        outs[index][pl.ds(rows, rows), :] = swapped_ref[pl.ds(index * rows, rows), :]
        outs[index][pl.ds(2 * rows, 8), :] = tile


def place_kernel(info, sources, tiles, order_ref, *refs):
    n_devices, chunks, total_len, device_id = info()
    ins = refs[:-4]
    out_ref, checks_ref, held, factor_ref = refs[-4:]
    group = pl.program_id(0)
    dev_bits = n_devices.bit_length() - 1
    chunk_bits = chunks.bit_length() - 1
    slot_rows = held.shape[0] // n_devices

    @pl.when(group == 0)
    def _():
        turned_id = jnp.int32(0)
        for bit in range(dev_bits):
            turned_id += (device_id >> bit & 1) << (dev_bits - 1 - bit)
        rows = chunks * RADIX * 8
        for mask, array, offset in sources:
            slot = turned_id ^ flip(mask, dev_bits)
            target = pl.ds(pl.multiple_of(slot * slot_rows, 8), rows)
            held[target, :] = ins[array][pl.ds(offset, rows), :]
        tile = jnp.zeros((8, LANES), jnp.float32)
        for array, offset in tiles:
            tile = tile + ins[array][pl.ds(offset, 8), :]
        sums = tile.sum(1, keepdims=True)
        mean_square = jnp.broadcast_to(sums[0:1], (8, LANES)) * (1.0 / total_len)
        shifted = mean_square + 1e-06
        factor = lax.rsqrt(shifted)
        factor = factor * (1.5 - 0.5 * shifted * factor * factor)
        factor_ref[...] = factor
        columns = 2**WINDOW
        scaled = factor * math.sqrt(columns / total_len)
        checks_ref[0] = mean_square[0, 0]
        checks_ref[1] = (jnp.broadcast_to(sums[1:2], (8, LANES)) * scaled)[0, 0]
        checks_ref[2] = (jnp.broadcast_to(sums[2:3], (8, LANES)) * scaled)[0, 0]

    factor = jnp.broadcast_to(factor_ref[0:1], (LANES, LANES))
    order = order_ref[...]
    for residue in range(RADIX):
        for part in range(2):
            pieces = []
            for low in range(chunks):
                tile_row = (flip(low, chunk_bits) * RADIX + residue) * 8 + part
                pieces.append(held[pl.ds(tile_row + 2 * group, n_devices, stride=slot_rows), :])
            high, low = halves(jnp.concatenate(pieces, 0))
            turned = dot_rows(order, jnp.concatenate([high, low], 1))
            out_ref[pl.ds(residue * 2 * LANES + part, LANES, stride=2), :] = turned * factor


def reverse_index(values, count):
    result = jnp.zeros_like(values)
    for bit_pos in range(count):
        result = result | (values >> bit_pos & 1) << count - 1 - bit_pos
    return result


def reversal_table(size, count):
    indices = jnp.arange(size, dtype=jnp.int32)
    return (reverse_index(indices, count)[:, None] == indices[None, :]).astype(jnp.float32)


def check_terms(current, positions, angle_scale):
    angles = positions.astype(jnp.float32) * angle_scale
    cosine = jnp.cos(angles)
    sine = jnp.sin(angles)
    squares = jnp.sum(current * current)
    phase_real = jnp.sum(current[0] * cosine + current[1] * sine)
    phase_imag = jnp.sum(current[1] * cosine - current[0] * sine)
    return (squares, phase_real, phase_imag)


def general_device(amplitudes):
    amp_dev = amplitudes.shape[1]
    n_outer = lax.axis_size("outer")
    n_inner = lax.axis_size("inner")
    outer_bits = n_outer.bit_length() - 1
    inner_bits = n_inner.bit_length() - 1
    global_bits = outer_bits + inner_bits
    local_bits = amp_dev.bit_length() - 1
    n_devices = n_outer * n_inner
    high_count = amp_dev // n_devices
    total_len = amp_dev * n_devices
    columns = 2**WINDOW
    rows_count = amp_dev // columns
    column_ids = jnp.arange(columns, dtype=jnp.int32)
    reversed_ids = reverse_index(column_ids, WINDOW)
    products = column_ids[:, None] * reversed_ids[None, :] % columns
    angles = products.astype(jnp.float32) * (2.0 * math.pi / columns)
    real_part = jnp.cos(angles) / math.sqrt(columns)
    imag_part = jnp.sin(angles) / math.sqrt(columns)
    table = jnp.concatenate(
        [jnp.concatenate([real_part, imag_part], 1), jnp.concatenate([-imag_part, real_part], 1)], 0
    )
    stacked = jnp.concatenate(
        [amplitudes[0].reshape(rows_count, columns), amplitudes[1].reshape(rows_count, columns)], 1
    )
    result = jnp.dot(
        stacked, table, precision=lax.Precision.HIGHEST, preferred_element_type=jnp.float32
    )
    windowed = jnp.stack([result[:, :columns].reshape(-1), result[:, columns:].reshape(-1)])
    device_id = lax.axis_index("outer") * n_inner + lax.axis_index("inner")
    angle_scale = 2.0 * math.pi / total_len
    local_ids = jnp.arange(amp_dev, dtype=jnp.int32)
    positions = reverse_index(device_id * amp_dev + local_ids, local_bits + global_bits)
    totals = lax.psum(check_terms(windowed, positions, angle_scale), ("outer", "inner"))
    device_table = reversal_table(n_devices, global_bits)
    high_table = reversal_table(high_count, local_bits - global_bits)
    grid = windowed.reshape(2, high_count, n_devices)
    ordered = jnp.einsum("pm,shm->sph", device_table, grid, precision=lax.Precision.HIGHEST)
    blocks = ordered.reshape(2, n_outer, n_inner, high_count)
    blocks = lax.all_to_all(
        lax.all_to_all(blocks, "outer", split_axis=1, concat_axis=1, tiled=True),
        "inner",
        split_axis=2,
        concat_axis=2,
        tiled=True,
    )
    received = blocks.reshape(2, n_devices, high_count)
    turned_high = jnp.einsum("qh,sdh->sdq", high_table, received, precision=lax.Precision.HIGHEST)
    placed = jnp.einsum("ed,sdq->sqe", device_table, turned_high, precision=lax.Precision.HIGHEST)
    reversed_field = placed.reshape(2, amp_dev)
    mean_square = totals[0] / total_len
    factor = lax.rsqrt(mean_square + 1e-06)
    scaled = factor / math.sqrt(total_len)
    checks = jnp.stack([mean_square, totals[1] * scaled, totals[2] * scaled])
    return (reversed_field * factor, checks)


def per_device(amplitudes):
    amp_dev = amplitudes.shape[1]
    n_devices = lax.axis_size("outer") * lax.axis_size("inner")
    n_inner = lax.axis_size("inner")
    total_len = amp_dev * n_devices
    columns = 2**WINDOW
    rows_count = amp_dev // columns
    chunks = rows_count // LANES
    groups = columns // n_devices // RADIX
    if chunks * n_devices != LANES or groups * 2 != 8:
        return general_device(amplitudes)
    vectors = 2 * amp_dev // LANES
    slot_rows = chunks * RADIX * 8 + 8
    x = amplitudes.reshape(2, vectors // 2, LANES).transpose(1, 0, 2).reshape(vectors, LANES)
    high, low = transform_tables()
    turn = np.array([flip(lane, LANES.bit_length() - 1) for lane in range(LANES)])
    order = (turn[:, None] == np.arange(LANES)[None, :]).astype(np.float32)
    order = np.concatenate([order, order], 1).astype(ml_dtypes.bfloat16)
    turn_table = np.broadcast_to(turn[:, None], (LANES, LANES)).astype(np.float32)

    rows = chunks * RADIX * 8
    core_bit = n_inner
    far_bit = n_inner // 2
    weight = lambda mask: mask.bit_count()
    chip_masks = [mask for mask in range(n_devices) if not mask & core_bit]
    far = sorted([mask for mask in chip_masks if mask & far_bit], key=weight)
    near = sorted([mask for mask in chip_masks if mask and not mask & far_bit], key=weight)
    direct, pairs = far[:2], far[2:] + near
    n_pairs = len(pairs)

    def info():
        device_id = lax.axis_index("outer") * n_inner + lax.axis_index("inner")
        return n_devices, chunks, 2.0 * math.pi / total_len, device_id

    def place_info():
        return n_devices, chunks, total_len, info()[3]

    def exchange(values, mask):
        pairs_of = [(source, source ^ mask) for source in range(n_devices)]
        return lax.ppermute(values, AXES, pairs_of)

    singles = [mask ^ core for mask in direct for core in (0, core_bit)]
    swap_rows = (n_pairs + 1) * rows
    shapes = [(2 * rows + 8, LANES)] * n_pairs + [(rows + 8, LANES), (swap_rows + 8, LANES)]
    shapes += [(rows + 8, LANES)] * len(singles)
    stay, swap = n_pairs, n_pairs + 1
    targets = [(mask, index, 0) for index, mask in enumerate(pairs)] + [(0, stay, 0)]
    targets += [(mask ^ core_bit, swap, index * rows) for index, mask in enumerate(pairs + [0])]
    targets += [(mask, swap + 1 + index, 0) for index, mask in enumerate(singles)]
    tiles = [(stay, rows), (swap, swap_rows)]
    tiles += [(swap + 1 + index, rows) for index in range(len(singles))]
    whole = lambda shape: pl.BlockSpec(shape, lambda i: (0,) * len(shape))
    hbm = pl.BlockSpec(memory_space=pltpu.HBM)
    vmem = pl.BlockSpec(memory_space=pltpu.VMEM)
    sent = pl.pallas_call(
        lambda *refs: transform_kernel(info, targets, tiles, *refs),
        in_specs=[hbm] * 4,
        out_specs=[vmem] * len(shapes),
        out_shape=[jax.ShapeDtypeStruct(shape, jnp.float32) for shape in shapes],
        scratch_shapes=[
            pltpu.VMEM((vectors, LANES), jnp.float32),
            pltpu.VMEM(high.shape, jnp.bfloat16),
            pltpu.VMEM(low.shape, jnp.bfloat16),
            pltpu.VMEM(turn_table.shape, jnp.float32),
            pltpu.VMEM((n_devices, RADIX * 8, LANES), jnp.float32),
            pltpu.SemaphoreType.DMA((chunks + 1 + 2 * RADIX,)),
        ],
        compiler_params=pltpu.CompilerParams(vmem_limit_bytes=VMEM_LIMIT),
        name="transform",
    )(*[pltpu.with_memory_space_constraint(a, pltpu.HBM) for a in (x, jnp.asarray(high), jnp.asarray(low), jnp.asarray(turn_table))])
    swapped = exchange(sent[swap], core_bit)
    arrived_singles = []
    for index, mask in enumerate(singles):
        arrived_singles.append(exchange(sent[swap + 1 + index], mask))
    joined = pl.pallas_call(
        lambda *refs: join_kernel((rows, swap_rows), n_pairs, *refs),
        in_specs=[vmem] * (2 + n_pairs),
        out_specs=[vmem] * n_pairs,
        out_shape=[jax.ShapeDtypeStruct(shapes[0], jnp.float32)] * n_pairs,
        input_output_aliases={2 + i: i for i in range(n_pairs)},
        compiler_params=pltpu.CompilerParams(vmem_limit_bytes=VMEM_LIMIT),
        name="join",
    )(swapped, sent[stay], *sent[:n_pairs])
    arrived_pairs = []
    for index, mask in enumerate(pairs):
        arrived_pairs.append(exchange(joined[index], mask))
    arrivals = arrived_pairs + [sent[stay], swapped] + arrived_singles
    sources = []
    for index, mask in enumerate(pairs):
        sources += [(mask, index, 0), (mask ^ core_bit, index, rows)]
    sources += [(0, stay, 0), (core_bit, swap, n_pairs * rows)]
    sources += [(mask, swap + 1 + index, 0) for index, mask in enumerate(singles)]
    tiles = [(index, 2 * rows) for index in range(n_pairs)] + tiles
    placed, checks = pl.pallas_call(
        lambda *refs: place_kernel(place_info, sources, tiles, *refs),
        grid=(groups,),
        in_specs=[whole(order.shape)] + [vmem] * len(arrivals),
        out_specs=[
            pl.BlockSpec((vectors // groups, LANES), lambda i: (i, 0)),
            pl.BlockSpec(memory_space=pltpu.SMEM),
        ],
        out_shape=[
            jax.ShapeDtypeStruct((vectors, LANES), jnp.float32),
            jax.ShapeDtypeStruct((3,), jnp.float32),
        ],
        scratch_shapes=[
            pltpu.VMEM((n_devices * slot_rows, LANES), jnp.float32),
            pltpu.VMEM((8, LANES), jnp.float32),
        ],
        compiler_params=pltpu.CompilerParams(vmem_limit_bytes=VMEM_LIMIT),
        name="place",
    )(jnp.asarray(order), *arrivals)
    placed = placed.reshape(vectors // 2, 2, LANES).transpose(1, 0, 2).reshape(2, amp_dev)
    return placed, checks


def solution(mesh):
    return jax.shard_map(
        per_device,
        mesh=mesh,
        in_specs=(P(None, ("outer", "inner")),),
        out_specs=(P(None, ("outer", "inner")), P()),
        check_vma=False,
    )
```

```python
import math

import jax
import jax.numpy as jnp
import ml_dtypes
import numpy as np
from jax import lax
from jax.experimental import pallas as pl
from jax.experimental.pallas import tpu as pltpu
from jax.sharding import PartitionSpec as P


WINDOW = 9
LANES = 128
RADIX = 2**WINDOW // LANES
AXES = ("outer", "inner")
VMEM_LIMIT = 16 * 2**20
SUB = 32


def flip(value, count):
    result = 0
    for bit_pos in range(count):
        result |= (value >> bit_pos & 1) << count - 1 - bit_pos
    return result


def split_halves(table):
    high = table.astype(ml_dtypes.bfloat16)
    low = (table - high.astype(np.float64)).astype(ml_dtypes.bfloat16)
    return high, low


def transform_tables(n_devices):
    columns = 2**WINDOW
    freq = np.arange(LANES) * RADIX
    sample = np.arange(LANES)
    tables = []
    for residue in range(RADIX):
        angles = (freq + residue)[:, None] * sample[None, :] % columns * (2 * np.pi / columns)
        cosine = np.cos(angles) / math.sqrt(columns)
        sine = np.sin(angles) / math.sqrt(columns)
        rows = np.stack([np.concatenate([cosine, -sine], 1), np.concatenate([sine, cosine], 1)], 1)
        tables.append(rows.reshape(n_devices // 2, 2, 8, 2 * LANES))
    high, low = split_halves(np.stack(tables))
    both = np.concatenate([high, low], 0).transpose(1, 0, 2, 3, 4)
    both = np.stack([both, both[:, :, ::-1]])
    return both.reshape(2, n_devices // 2, 2 * RADIX, 16, 2 * LANES)


def phase_tables(chunks, n_devices, angle_scale):
    turn = np.array([flip(row, LANES.bit_length() - 1) for row in range(LANES)])
    angles = turn * float(chunks * n_devices) * angle_scale
    table = np.zeros((2, LANES, LANES))
    table[0, :, 1] = np.cos(angles)
    table[1, :, 1] = np.sin(angles)
    return table.astype(np.float32)


def halves(values):
    high = values.astype(jnp.bfloat16)
    low = (values - high.astype(jnp.float32)).astype(jnp.bfloat16)
    return high, low


def dot_rows(left, right):
    return lax.dot_general(
        left, right, (((1,), (1,)), ((), ())), preferred_element_type=jnp.float32
    )


def transform_kernel(info, targets, tiles, x_hbm, table_hbm, phase_hbm, *refs):
    n_devices, chunks, angle_scale, device_id = info()
    outs, (x_ref, table_ref, phase_ref, high_ref, low_ref, sems) = refs[:-6], refs[-6:]
    chunk_rows = RADIX * 8
    x_rows = x_ref.shape[0] // chunks
    dev_bits = n_devices.bit_length() - 1
    chunk_bits = chunks.bit_length() - 1

    def load(source, target, index):
        return pltpu.make_async_copy(source, target, sems.at[index])

    loads = []
    for chunk in range(chunks):
        rows = pl.ds(chunk * x_rows, x_rows)
        loads.append(load(x_hbm.at[rows], x_ref.at[rows], chunk))
    phase_load = load(phase_hbm, phase_ref, chunks)
    table_loads = [
        load(
            table_hbm.at[device_id & 1, (device_id >> 1) ^ block],
            table_ref.at[block],
            chunks + 1 + block,
        )
        for block in range(n_devices // 2)
    ]
    for copy in loads[:1] + [phase_load] + loads[1:2] + table_loads + loads[2:]:
        copy.start()

    base = jnp.int32(0)
    for bit in range(dev_bits):
        base += (device_id >> bit & 1) << (dev_bits - 1 - bit)
    square_sum = real_sum = imag_sum = jnp.zeros((8, LANES), jnp.float32)
    fold = lambda value: value.reshape(SUB // 8, 8, LANES).sum(0)
    for half in range(chunks // 2):
        for chunk in (2 * half, 2 * half + 1):
            loads[chunk].wait()
            if chunk == 0:
                phase_load.wait()
            turn_re = turn_im = jnp.zeros((8, LANES), jnp.float32)
            for sub in range(LANES // SUB):
                start = chunk * x_rows + sub * SUB * 2 * RADIX
                parts = [
                    [x_ref[pl.ds(start + 2 * j + s, SUB, stride=2 * RADIX), :] for s in range(2)]
                    for j in range(RADIX)
                ]
                square_sum += fold(sum(p * p for pair in parts for p in pair))
                cosine = phase_ref[0, sub * SUB : (sub + 1) * SUB]
                sine = phase_ref[1, sub * SUB : (sub + 1) * SUB]
                first_re, first_im = parts[0]
                turn_re += fold(first_re * cosine + first_im * sine)
                turn_im += fold(first_im * cosine - first_re * sine)
                (r0, i0), (r1, i1), (r2, i2), (r3, i3) = parts
                ar, ai, br, bi = r0 + r2, i0 + i2, r0 - r2, i0 - i2
                cr, ci, dr, di = r1 + r3, i1 + i3, r1 - r3, i1 - i3
                folded = [
                    (ar + cr, ai + ci),
                    (br - di, bi + dr),
                    (ar - cr, ai - ci),
                    (br + di, bi - dr),
                ]
                row = (chunk % 2) * LANES + sub * SUB
                for residue in range(RADIX):
                    for part in range(2):
                        high, low = halves(folded[residue][part])
                        where = (residue, pl.ds(row, SUB), pl.ds(part * LANES, LANES))
                        high_ref[where] = high
                        low_ref[where] = low
            angle = flip(chunk, chunk_bits) * n_devices * angle_scale
            cosine, sine = math.cos(angle), math.sin(angle)
            real_sum += turn_re * cosine + turn_im * sine
            imag_sum += turn_im * cosine - turn_re * sine
        if half == 0:
            for copy in table_loads:
                copy.wait()
        for residue in range(RADIX):
            table_high = table_ref[:, residue].reshape(2 * LANES, 2 * LANES)
            table_low = table_ref[:, RADIX + residue].reshape(2 * LANES, 2 * LANES)
            high, low = high_ref[residue], low_ref[residue]
            values = dot_rows(table_high, high) + dot_rows(table_high, low)
            values += dot_rows(table_low, high)
            for mask, out, row in targets:
                for part in range(2):
                    rows = pl.ds(row + (2 * half + part) * chunk_rows + residue * 8, 8)
                    outs[out][rows, :] = values[
                        8 * mask : 8 * mask + 8, part * LANES : (part + 1) * LANES
                    ]

    theta = jnp.full((8, LANES), base, jnp.int32).astype(jnp.float32) * angle_scale
    theta_sq = theta * theta
    cosine = 1.0 - theta_sq * (0.5 - theta_sq * (1.0 / 24.0))
    sine = theta * (1.0 - theta_sq * (1.0 / 6.0 - theta_sq * (1.0 / 120.0)))
    turned = (square_sum, real_sum * cosine + imag_sum * sine, imag_sum * cosine - real_sum * sine)
    sums = [value.sum(0, keepdims=True) for value in turned]
    tile = jnp.concatenate(sums + [jnp.zeros((5, LANES), jnp.float32)], 0)
    for out, row in tiles:
        outs[out][pl.ds(row, 8), :] = tile


def join_kernel(rows, first, stamps, n_join, swapped_ref, *refs):
    refs = (swapped_ref,) + refs
    outs = refs[len(refs) - n_join :]
    tile = None
    for operand, row in stamps:
        value = refs[operand][pl.ds(row, 8), :]
        tile = value if tile is None else tile + value
    for index, out in enumerate(outs):
        out[pl.ds(rows, rows), :] = swapped_ref[pl.ds((first + index) * rows, rows), :]
        if tile is not None:
            out[pl.ds(2 * rows, 8), :] = tile


def place_kernel(info, sources, tiles, order_ref, *refs):
    n_devices, chunks, total_len, device_id = info()
    ins = refs[:-4]
    out_ref, checks_ref, held, factor_ref = refs[-4:]
    group = pl.program_id(0)
    dev_bits = n_devices.bit_length() - 1
    chunk_bits = chunks.bit_length() - 1
    slot_rows = held.shape[0] // n_devices

    @pl.when(group == 0)
    def _():
        turned_id = jnp.int32(0)
        for bit in range(dev_bits):
            turned_id += (device_id >> bit & 1) << (dev_bits - 1 - bit)
        rows = chunks * RADIX * 8
        for mask, array, offset in sources:
            slot = turned_id ^ flip(mask, dev_bits)
            target = pl.ds(pl.multiple_of(slot * slot_rows, 8), rows)
            held[target, :] = ins[array][pl.ds(offset, rows), :]
        tile = jnp.zeros((8, LANES), jnp.float32)
        for array, offset in tiles:
            tile = tile + ins[array][pl.ds(offset, 8), :]
        sums = tile.sum(1, keepdims=True)
        mean_square = jnp.broadcast_to(sums[0:1], (8, LANES)) * (1.0 / total_len)
        shifted = mean_square + 1e-06
        factor = lax.rsqrt(shifted)
        factor = factor * (1.5 - 0.5 * shifted * factor * factor)
        factor_ref[...] = factor
        columns = 2**WINDOW
        scaled = factor * math.sqrt(columns / total_len)
        checks_ref[0] = mean_square[0, 0]
        checks_ref[1] = (jnp.broadcast_to(sums[1:2], (8, LANES)) * scaled)[0, 0]
        checks_ref[2] = (jnp.broadcast_to(sums[2:3], (8, LANES)) * scaled)[0, 0]

    factor = jnp.broadcast_to(factor_ref[0:1], (LANES, LANES))
    order = order_ref[...]
    for residue in range(RADIX):
        for part in range(2):
            pieces = []
            for low in range(chunks):
                tile_row = (flip(low, chunk_bits) * RADIX + residue) * 8 + part
                pieces.append(held[pl.ds(tile_row + 2 * group, n_devices, stride=slot_rows), :])
            high, low = halves(jnp.concatenate(pieces, 0))
            turned = dot_rows(order, jnp.concatenate([high, low], 1))
            out_ref[pl.ds(residue * 2 * LANES + part, LANES, stride=2), :] = turned * factor


def reverse_index(values, count):
    result = jnp.zeros_like(values)
    for bit_pos in range(count):
        result = result | (values >> bit_pos & 1) << count - 1 - bit_pos
    return result


def reversal_table(size, count):
    indices = jnp.arange(size, dtype=jnp.int32)
    return (reverse_index(indices, count)[:, None] == indices[None, :]).astype(jnp.float32)


def check_terms(current, positions, angle_scale):
    angles = positions.astype(jnp.float32) * angle_scale
    cosine = jnp.cos(angles)
    sine = jnp.sin(angles)
    squares = jnp.sum(current * current)
    phase_real = jnp.sum(current[0] * cosine + current[1] * sine)
    phase_imag = jnp.sum(current[1] * cosine - current[0] * sine)
    return (squares, phase_real, phase_imag)


def general_device(amplitudes):
    amp_dev = amplitudes.shape[1]
    n_outer = lax.axis_size("outer")
    n_inner = lax.axis_size("inner")
    outer_bits = n_outer.bit_length() - 1
    inner_bits = n_inner.bit_length() - 1
    global_bits = outer_bits + inner_bits
    local_bits = amp_dev.bit_length() - 1
    n_devices = n_outer * n_inner
    high_count = amp_dev // n_devices
    total_len = amp_dev * n_devices
    columns = 2**WINDOW
    rows_count = amp_dev // columns
    column_ids = jnp.arange(columns, dtype=jnp.int32)
    reversed_ids = reverse_index(column_ids, WINDOW)
    products = column_ids[:, None] * reversed_ids[None, :] % columns
    angles = products.astype(jnp.float32) * (2.0 * math.pi / columns)
    real_part = jnp.cos(angles) / math.sqrt(columns)
    imag_part = jnp.sin(angles) / math.sqrt(columns)
    table = jnp.concatenate(
        [jnp.concatenate([real_part, imag_part], 1), jnp.concatenate([-imag_part, real_part], 1)], 0
    )
    stacked = jnp.concatenate(
        [amplitudes[0].reshape(rows_count, columns), amplitudes[1].reshape(rows_count, columns)], 1
    )
    result = jnp.dot(
        stacked, table, precision=lax.Precision.HIGHEST, preferred_element_type=jnp.float32
    )
    windowed = jnp.stack([result[:, :columns].reshape(-1), result[:, columns:].reshape(-1)])
    device_id = lax.axis_index("outer") * n_inner + lax.axis_index("inner")
    angle_scale = 2.0 * math.pi / total_len
    local_ids = jnp.arange(amp_dev, dtype=jnp.int32)
    positions = reverse_index(device_id * amp_dev + local_ids, local_bits + global_bits)
    totals = lax.psum(check_terms(windowed, positions, angle_scale), ("outer", "inner"))
    device_table = reversal_table(n_devices, global_bits)
    high_table = reversal_table(high_count, local_bits - global_bits)
    grid = windowed.reshape(2, high_count, n_devices)
    ordered = jnp.einsum("pm,shm->sph", device_table, grid, precision=lax.Precision.HIGHEST)
    blocks = ordered.reshape(2, n_outer, n_inner, high_count)
    blocks = lax.all_to_all(
        lax.all_to_all(blocks, "outer", split_axis=1, concat_axis=1, tiled=True),
        "inner",
        split_axis=2,
        concat_axis=2,
        tiled=True,
    )
    received = blocks.reshape(2, n_devices, high_count)
    turned_high = jnp.einsum("qh,sdh->sdq", high_table, received, precision=lax.Precision.HIGHEST)
    placed = jnp.einsum("ed,sdq->sqe", device_table, turned_high, precision=lax.Precision.HIGHEST)
    reversed_field = placed.reshape(2, amp_dev)
    mean_square = totals[0] / total_len
    factor = lax.rsqrt(mean_square + 1e-06)
    scaled = factor / math.sqrt(total_len)
    checks = jnp.stack([mean_square, totals[1] * scaled, totals[2] * scaled])
    return (reversed_field * factor, checks)


def per_device(amplitudes):
    amp_dev = amplitudes.shape[1]
    n_devices = lax.axis_size("outer") * lax.axis_size("inner")
    n_inner = lax.axis_size("inner")
    total_len = amp_dev * n_devices
    columns = 2**WINDOW
    rows_count = amp_dev // columns
    chunks = rows_count // LANES
    groups = columns // n_devices // RADIX
    if chunks * n_devices != LANES or groups * 2 != 8:
        return general_device(amplitudes)
    vectors = 2 * amp_dev // LANES
    slot_rows = chunks * RADIX * 8 + 8
    x = amplitudes.reshape(2, vectors // 2, LANES).transpose(1, 0, 2).reshape(vectors, LANES)
    angle_scale = 2.0 * math.pi / total_len
    table = transform_tables(n_devices)
    phase = phase_tables(chunks, n_devices, angle_scale)
    turn = np.array([flip(lane, LANES.bit_length() - 1) for lane in range(LANES)])
    order = (turn[:, None] == np.arange(LANES)[None, :]).astype(np.float32)
    order = np.concatenate([order, order], 1).astype(ml_dtypes.bfloat16)

    rows = chunks * RADIX * 8
    core_bit = n_inner
    far_bit = n_inner // 2
    weight = lambda mask: mask.bit_count()
    chip_masks = [mask for mask in range(n_devices) if not mask & core_bit]
    far = sorted([mask for mask in chip_masks if mask & far_bit], key=weight)
    near = sorted([mask for mask in chip_masks if mask and not mask & far_bit], key=weight)
    direct, far = far[:2], far[2:]
    pairs = far + near
    n_pairs = len(pairs)

    def info():
        device_id = lax.axis_index("outer") * n_inner + lax.axis_index("inner")
        return n_devices, chunks, angle_scale, device_id

    def place_info():
        return n_devices, chunks, total_len, info()[3]

    def exchange(values, mask):
        pairs_of = [(source, source ^ mask) for source in range(n_devices)]
        return lax.ppermute(values, AXES, pairs_of)

    singles = [mask ^ core for mask in direct for core in (0, core_bit)]
    swap_rows = (n_pairs + 1) * rows
    pair_rows = [2 * rows] * len(far) + [2 * rows + 8] * len(near)
    single_rows = [rows + 8] * 2 + [rows] * (len(singles) - 2)
    all_rows = pair_rows + [rows + 8, swap_rows + 8] + single_rows
    stay, swap = n_pairs, n_pairs + 1
    targets = [(mask, index, 0) for index, mask in enumerate(pairs)] + [(0, stay, 0)]
    targets += [(mask ^ core_bit, swap, index * rows) for index, mask in enumerate(pairs + [0])]
    targets += [(mask, swap + 1 + index, 0) for index, mask in enumerate(singles)]
    tiles = [(stay, rows), (swap, swap_rows), (swap + 1, rows), (swap + 2, rows)]
    constrain = lambda value: pltpu.with_memory_space_constraint(value, pltpu.HBM)
    shaped = lambda count: jax.ShapeDtypeStruct((count, LANES), jnp.float32)
    whole = lambda shape: pl.BlockSpec(shape, lambda i: (0,) * len(shape))
    hbm = pl.BlockSpec(memory_space=pltpu.HBM)
    vmem = pl.BlockSpec(memory_space=pltpu.VMEM)
    sent = pl.pallas_call(
        lambda *refs: transform_kernel(info, targets, tiles, *refs),
        in_specs=[hbm] * 3,
        out_specs=[vmem] * len(all_rows),
        out_shape=[shaped(count) for count in all_rows],
        scratch_shapes=[
            pltpu.VMEM((vectors, LANES), jnp.float32),
            pltpu.VMEM(table.shape[1:], jnp.bfloat16),
            pltpu.VMEM(phase.shape, jnp.float32),
            pltpu.VMEM((RADIX, 2 * LANES, 2 * LANES), jnp.bfloat16),
            pltpu.VMEM((RADIX, 2 * LANES, 2 * LANES), jnp.bfloat16),
            pltpu.SemaphoreType.DMA((chunks + 1 + n_devices // 2,)),
        ],
        compiler_params=pltpu.CompilerParams(vmem_limit_bytes=VMEM_LIMIT),
        name="transform",
    )(constrain(x), constrain(jnp.asarray(table)), constrain(jnp.asarray(phase)))
    swapped = exchange(sent[swap], core_bit)
    arrived_singles = []
    for index, mask in enumerate(singles):
        arrived_singles.append(exchange(sent[swap + 1 + index], mask))

    def join(first, count, extra, stamps):
        n_extra = len(extra)
        return pl.pallas_call(
            lambda *refs: join_kernel(rows, first, stamps, count, *refs),
            in_specs=[vmem] * (1 + n_extra + count),
            out_specs=[vmem] * count,
            out_shape=[shaped(size) for size in pair_rows[first : first + count]],
            input_output_aliases={1 + n_extra + i: i for i in range(count)},
            compiler_params=pltpu.CompilerParams(vmem_limit_bytes=VMEM_LIMIT),
            name="join",
        )(swapped, *extra, *sent[first : first + count])

    joined = join(0, len(far), [], [])
    stamps = [(0, swap_rows), (1, rows), (2, rows), (3, rows)]
    joined += join(len(far), len(near), [sent[stay]] + arrived_singles[:2], stamps)
    arrived_pairs = []
    for index, mask in enumerate(pairs):
        arrived_pairs.append(exchange(joined[index], mask))
    arrivals = arrived_pairs + [sent[stay], swapped] + arrived_singles
    sources = []
    for index, mask in enumerate(pairs):
        sources += [(mask, index, 0), (mask ^ core_bit, index, rows)]
    sources += [(0, stay, 0), (core_bit, swap, n_pairs * rows)]
    sources += [(mask, swap + 1 + index, 0) for index, mask in enumerate(singles)]
    sums = tiles + [(len(far) + index, 2 * rows) for index in range(len(near))]
    placed, checks = pl.pallas_call(
        lambda *refs: place_kernel(place_info, sources, sums, *refs),
        grid=(groups,),
        in_specs=[whole(order.shape)] + [vmem] * len(arrivals),
        out_specs=[
            pl.BlockSpec((vectors // groups, LANES), lambda i: (i, 0)),
            pl.BlockSpec(memory_space=pltpu.SMEM),
        ],
        out_shape=[
            jax.ShapeDtypeStruct((vectors, LANES), jnp.float32),
            jax.ShapeDtypeStruct((3,), jnp.float32),
        ],
        scratch_shapes=[
            pltpu.VMEM((n_devices * slot_rows, LANES), jnp.float32),
            pltpu.VMEM((8, LANES), jnp.float32),
        ],
        compiler_params=pltpu.CompilerParams(vmem_limit_bytes=VMEM_LIMIT),
        name="place",
    )(jnp.asarray(order), *arrivals)
    placed = placed.reshape(vectors // 2, 2, LANES).transpose(1, 0, 2).reshape(2, amp_dev)
    return placed, checks


def solution(mesh):
    return jax.shard_map(
        per_device,
        mesh=mesh,
        in_specs=(P(None, ("outer", "inner")),),
        out_specs=(P(None, ("outer", "inner")), P()),
        check_vma=False,
    )
```

```python
import math

import jax
import jax.numpy as jnp
import ml_dtypes
import numpy as np
from jax import lax
from jax.experimental import pallas as pl
from jax.experimental.pallas import tpu as pltpu
from jax.sharding import PartitionSpec as P


WINDOW = 9
LANES = 128
RADIX = 2**WINDOW // LANES
AXES = ("outer", "inner")
VMEM_LIMIT = 16 * 2**20
SUB = 16


def flip(value, count):
    result = 0
    for bit_pos in range(count):
        result |= (value >> bit_pos & 1) << count - 1 - bit_pos
    return result


def split_halves(table):
    high = table.astype(ml_dtypes.bfloat16)
    low = (table - high.astype(np.float64)).astype(ml_dtypes.bfloat16)
    return high, low


def transform_tables(n_devices):
    columns = 2**WINDOW
    freq = np.arange(LANES) * RADIX
    sample = np.arange(LANES)
    tables = []
    for residue in range(RADIX):
        angles = (freq + residue)[:, None] * sample[None, :] % columns * (2 * np.pi / columns)
        cosine = np.cos(angles) / math.sqrt(columns)
        sine = np.sin(angles) / math.sqrt(columns)
        rows = np.stack([np.concatenate([cosine, -sine], 1), np.concatenate([sine, cosine], 1)], 1)
        tables.append(rows.reshape(n_devices // 2, 2, 8, 2 * LANES))
    high, low = split_halves(np.stack(tables))
    both = np.concatenate([high, low], 0).transpose(1, 0, 2, 3, 4)
    both = np.stack([both, both[:, :, ::-1]])
    return both.reshape(2, n_devices // 2, 2 * RADIX, 16, 2 * LANES)


def phase_tables(chunks, n_devices, angle_scale):
    turn = np.array([flip(row, LANES.bit_length() - 1) for row in range(LANES)])
    angles = turn * float(chunks * n_devices) * angle_scale
    table = np.zeros((2, LANES, LANES))
    table[0, :, 1] = np.cos(angles)
    table[1, :, 1] = np.sin(angles)
    return table.astype(np.float32)


def halves(values):
    high = values.astype(jnp.bfloat16)
    low = (values - high.astype(jnp.float32)).astype(jnp.bfloat16)
    return high, low


def dot_rows(left, right):
    return lax.dot_general(
        left, right, (((1,), (1,)), ((), ())), preferred_element_type=jnp.float32
    )


def transform_kernel(info, targets, tiles, x_hbm, table_hbm, phase_hbm, *refs):
    n_devices, chunks, angle_scale, device_id = info()
    outs, (x_ref, table_ref, phase_ref, high_ref, low_ref, sems) = refs[:-6], refs[-6:]
    chunk_rows = RADIX * 8
    x_rows = x_ref.shape[0] // chunks
    dev_bits = n_devices.bit_length() - 1
    chunk_bits = chunks.bit_length() - 1

    def load(source, target, index):
        return pltpu.make_async_copy(source, target, sems.at[index])

    loads = []
    for chunk in range(chunks):
        rows = pl.ds(chunk * x_rows, x_rows)
        loads.append(load(x_hbm.at[rows], x_ref.at[rows], chunk))
    phase_load = load(phase_hbm, phase_ref, chunks)
    table_loads = [
        load(
            table_hbm.at[device_id & 1, (device_id >> 1) ^ block],
            table_ref.at[block],
            chunks + 1 + block,
        )
        for block in range(n_devices // 2)
    ]
    for copy in loads[:1] + [phase_load] + loads[1:] + table_loads:
        copy.start()

    base = jnp.int32(0)
    for bit in range(dev_bits):
        base += (device_id >> bit & 1) << (dev_bits - 1 - bit)
    square_sum = real_sum = imag_sum = jnp.zeros((8, LANES), jnp.float32)
    fold = lambda value: value.reshape(SUB // 8, 8, LANES).sum(0)
    for half in range(chunks // 2):
        for chunk in (2 * half, 2 * half + 1):
            loads[chunk].wait()
            if chunk == 0:
                phase_load.wait()
            turn_re = turn_im = jnp.zeros((8, LANES), jnp.float32)
            for sub in range(LANES // SUB):
                start = chunk * x_rows + sub * SUB * 2 * RADIX
                parts = [
                    [x_ref[pl.ds(start + 2 * j + s, SUB, stride=2 * RADIX), :] for s in range(2)]
                    for j in range(RADIX)
                ]
                square_sum += fold(sum(p * p for pair in parts for p in pair))
                cosine = phase_ref[0, sub * SUB : (sub + 1) * SUB]
                sine = phase_ref[1, sub * SUB : (sub + 1) * SUB]
                first_re, first_im = parts[0]
                turn_re += fold(first_re * cosine + first_im * sine)
                turn_im += fold(first_im * cosine - first_re * sine)
                (r0, i0), (r1, i1), (r2, i2), (r3, i3) = parts
                ar, ai, br, bi = r0 + r2, i0 + i2, r0 - r2, i0 - i2
                cr, ci, dr, di = r1 + r3, i1 + i3, r1 - r3, i1 - i3
                folded = [
                    (ar + cr, ai + ci),
                    (br - di, bi + dr),
                    (ar - cr, ai - ci),
                    (br + di, bi - dr),
                ]
                row = (chunk % 2) * LANES + sub * SUB
                for residue in range(RADIX):
                    for part in range(2):
                        high, low = halves(folded[residue][part])
                        where = (half, residue, pl.ds(row, SUB), pl.ds(part * LANES, LANES))
                        high_ref[where] = high
                        low_ref[where] = low
            angle = flip(chunk, chunk_bits) * n_devices * angle_scale
            cosine, sine = math.cos(angle), math.sin(angle)
            real_sum += turn_re * cosine + turn_im * sine
            imag_sum += turn_im * cosine - turn_re * sine
    for copy in table_loads:
        copy.wait()
    for half in range(chunks // 2):
        for residue in range(RADIX):
            table_high = table_ref[:, residue].reshape(2 * LANES, 2 * LANES)
            table_low = table_ref[:, RADIX + residue].reshape(2 * LANES, 2 * LANES)
            high, low = high_ref[half, residue], low_ref[half, residue]
            values = dot_rows(table_high, high) + dot_rows(table_high, low)
            values += dot_rows(table_low, high)
            for mask, out, row in targets:
                for part in range(2):
                    rows = pl.ds(row + (2 * half + part) * chunk_rows + residue * 8, 8)
                    outs[out][rows, :] = values[
                        8 * mask : 8 * mask + 8, part * LANES : (part + 1) * LANES
                    ]

    theta = jnp.full((8, LANES), base, jnp.int32).astype(jnp.float32) * angle_scale
    theta_sq = theta * theta
    cosine = 1.0 - theta_sq * (0.5 - theta_sq * (1.0 / 24.0))
    sine = theta * (1.0 - theta_sq * (1.0 / 6.0 - theta_sq * (1.0 / 120.0)))
    turned = (square_sum, real_sum * cosine + imag_sum * sine, imag_sum * cosine - real_sum * sine)
    sums = [value.sum(0, keepdims=True) for value in turned]
    tile = jnp.concatenate(sums + [jnp.zeros((5, LANES), jnp.float32)], 0)
    for out, row in tiles:
        outs[out][pl.ds(row, 8), :] = tile


def join_kernel(rows, first, stamps, n_join, swapped_ref, *refs):
    refs = (swapped_ref,) + refs
    outs = refs[len(refs) - n_join :]
    tile = None
    for operand, row in stamps:
        value = refs[operand][pl.ds(row, 8), :]
        tile = value if tile is None else tile + value
    for index, out in enumerate(outs):
        out[pl.ds(rows, rows), :] = swapped_ref[pl.ds((first + index) * rows, rows), :]
        if tile is not None:
            out[pl.ds(2 * rows, 8), :] = tile


def place_kernel(info, sources, tiles, order_ref, *refs):
    n_devices, chunks, groups, total_len, device_id = info()
    ins = refs[:-5]
    out_hbm, checks_ref, held, out_ref, sems = refs[-5:]
    dev_bits = n_devices.bit_length() - 1
    chunk_bits = chunks.bit_length() - 1
    slot_rows = held.shape[0] // n_devices

    turned_id = jnp.int32(0)
    for bit in range(dev_bits):
        turned_id += (device_id >> bit & 1) << (dev_bits - 1 - bit)
    rows = chunks * RADIX * 8
    for mask, array, offset in sources:
        slot = turned_id ^ flip(mask, dev_bits)
        target = pl.ds(pl.multiple_of(slot * slot_rows, 8), rows)
        held[target, :] = ins[array][pl.ds(offset, rows), :]
    tile = jnp.zeros((8, LANES), jnp.float32)
    for array, offset in tiles:
        tile = tile + ins[array][pl.ds(offset, 8), :]
    sums = tile.sum(1, keepdims=True)
    mean_square = jnp.broadcast_to(sums[0:1], (8, LANES)) * (1.0 / total_len)
    shifted = mean_square + 1e-06
    factor = lax.rsqrt(shifted)
    factor = factor * (1.5 - 0.5 * shifted * factor * factor)
    columns = 2**WINDOW
    scaled = factor * math.sqrt(columns / total_len)
    checks_ref[0] = mean_square[0, 0]
    checks_ref[1] = (jnp.broadcast_to(sums[1:2], (8, LANES)) * scaled)[0, 0]
    checks_ref[2] = (jnp.broadcast_to(sums[2:3], (8, LANES)) * scaled)[0, 0]

    factor = jnp.broadcast_to(factor[0:1], (LANES, LANES))
    order = order_ref[...]
    copies = []
    for group in range(groups):
        for residue in range(RADIX):
            for part in range(2):
                pieces = []
                for low in range(chunks):
                    tile_row = (flip(low, chunk_bits) * RADIX + residue) * 8 + 2 * group + part
                    pieces.append(held[pl.ds(tile_row, n_devices, stride=slot_rows), :])
                high, low = halves(jnp.concatenate(pieces, 0))
                turned = dot_rows(order, jnp.concatenate([high, low], 1))
                row = (group * RADIX + residue) * 2 * LANES + part
                out_ref[pl.ds(row, LANES, stride=2), :] = turned * factor
        size = RADIX * 2 * LANES
        span = pl.ds(group * size, size)
        copies.append(pltpu.make_async_copy(out_ref.at[span], out_hbm.at[span], sems.at[group]))
        copies[-1].start()
    for copy in copies:
        copy.wait()


def reverse_index(values, count):
    result = jnp.zeros_like(values)
    for bit_pos in range(count):
        result = result | (values >> bit_pos & 1) << count - 1 - bit_pos
    return result


def reversal_table(size, count):
    indices = jnp.arange(size, dtype=jnp.int32)
    return (reverse_index(indices, count)[:, None] == indices[None, :]).astype(jnp.float32)


def check_terms(current, positions, angle_scale):
    angles = positions.astype(jnp.float32) * angle_scale
    cosine = jnp.cos(angles)
    sine = jnp.sin(angles)
    squares = jnp.sum(current * current)
    phase_real = jnp.sum(current[0] * cosine + current[1] * sine)
    phase_imag = jnp.sum(current[1] * cosine - current[0] * sine)
    return (squares, phase_real, phase_imag)


def general_device(amplitudes):
    amp_dev = amplitudes.shape[1]
    n_outer = lax.axis_size("outer")
    n_inner = lax.axis_size("inner")
    outer_bits = n_outer.bit_length() - 1
    inner_bits = n_inner.bit_length() - 1
    global_bits = outer_bits + inner_bits
    local_bits = amp_dev.bit_length() - 1
    n_devices = n_outer * n_inner
    high_count = amp_dev // n_devices
    total_len = amp_dev * n_devices
    columns = 2**WINDOW
    rows_count = amp_dev // columns
    column_ids = jnp.arange(columns, dtype=jnp.int32)
    reversed_ids = reverse_index(column_ids, WINDOW)
    products = column_ids[:, None] * reversed_ids[None, :] % columns
    angles = products.astype(jnp.float32) * (2.0 * math.pi / columns)
    real_part = jnp.cos(angles) / math.sqrt(columns)
    imag_part = jnp.sin(angles) / math.sqrt(columns)
    table = jnp.concatenate(
        [jnp.concatenate([real_part, imag_part], 1), jnp.concatenate([-imag_part, real_part], 1)], 0
    )
    stacked = jnp.concatenate(
        [amplitudes[0].reshape(rows_count, columns), amplitudes[1].reshape(rows_count, columns)], 1
    )
    result = jnp.dot(
        stacked, table, precision=lax.Precision.HIGHEST, preferred_element_type=jnp.float32
    )
    windowed = jnp.stack([result[:, :columns].reshape(-1), result[:, columns:].reshape(-1)])
    device_id = lax.axis_index("outer") * n_inner + lax.axis_index("inner")
    angle_scale = 2.0 * math.pi / total_len
    local_ids = jnp.arange(amp_dev, dtype=jnp.int32)
    positions = reverse_index(device_id * amp_dev + local_ids, local_bits + global_bits)
    totals = lax.psum(check_terms(windowed, positions, angle_scale), ("outer", "inner"))
    device_table = reversal_table(n_devices, global_bits)
    high_table = reversal_table(high_count, local_bits - global_bits)
    grid = windowed.reshape(2, high_count, n_devices)
    ordered = jnp.einsum("pm,shm->sph", device_table, grid, precision=lax.Precision.HIGHEST)
    blocks = ordered.reshape(2, n_outer, n_inner, high_count)
    blocks = lax.all_to_all(
        lax.all_to_all(blocks, "outer", split_axis=1, concat_axis=1, tiled=True),
        "inner",
        split_axis=2,
        concat_axis=2,
        tiled=True,
    )
    received = blocks.reshape(2, n_devices, high_count)
    turned_high = jnp.einsum("qh,sdh->sdq", high_table, received, precision=lax.Precision.HIGHEST)
    placed = jnp.einsum("ed,sdq->sqe", device_table, turned_high, precision=lax.Precision.HIGHEST)
    reversed_field = placed.reshape(2, amp_dev)
    mean_square = totals[0] / total_len
    factor = lax.rsqrt(mean_square + 1e-06)
    scaled = factor / math.sqrt(total_len)
    checks = jnp.stack([mean_square, totals[1] * scaled, totals[2] * scaled])
    return (reversed_field * factor, checks)


def per_device(amplitudes):
    amp_dev = amplitudes.shape[1]
    n_devices = lax.axis_size("outer") * lax.axis_size("inner")
    n_inner = lax.axis_size("inner")
    total_len = amp_dev * n_devices
    columns = 2**WINDOW
    rows_count = amp_dev // columns
    chunks = rows_count // LANES
    groups = columns // n_devices // RADIX
    if chunks * n_devices != LANES or groups * 2 != 8:
        return general_device(amplitudes)
    vectors = 2 * amp_dev // LANES
    slot_rows = chunks * RADIX * 8 + 8
    x = amplitudes.reshape(2, vectors // 2, LANES).transpose(1, 0, 2).reshape(vectors, LANES)
    angle_scale = 2.0 * math.pi / total_len
    table = transform_tables(n_devices)
    phase = phase_tables(chunks, n_devices, angle_scale)
    turn = np.array([flip(lane, LANES.bit_length() - 1) for lane in range(LANES)])
    order = (turn[:, None] == np.arange(LANES)[None, :]).astype(np.float32)
    order = np.concatenate([order, order], 1).astype(ml_dtypes.bfloat16)

    rows = chunks * RADIX * 8
    core_bit = n_inner
    far_bit = n_inner // 2
    weight = lambda mask: mask.bit_count()
    chip_masks = [mask for mask in range(n_devices) if not mask & core_bit]
    far = sorted([mask for mask in chip_masks if mask & far_bit], key=weight)
    near = sorted([mask for mask in chip_masks if mask and not mask & far_bit], key=weight)
    direct, far = far[:2], far[2:]
    pairs = far + near
    n_pairs = len(pairs)

    def info():
        device_id = lax.axis_index("outer") * n_inner + lax.axis_index("inner")
        return n_devices, chunks, angle_scale, device_id

    def place_info():
        return n_devices, chunks, groups, total_len, info()[3]

    def exchange(values, mask):
        pairs_of = [(source, source ^ mask) for source in range(n_devices)]
        return lax.ppermute(values, AXES, pairs_of)

    singles = [mask ^ core for mask in direct for core in (0, core_bit)]
    swap_rows = (n_pairs + 1) * rows
    pair_rows = [2 * rows] * len(far) + [2 * rows + 8] * len(near)
    single_rows = [rows + 8] * 2 + [rows] * (len(singles) - 2)
    all_rows = pair_rows + [rows + 8, swap_rows + 8] + single_rows
    stay, swap = n_pairs, n_pairs + 1
    targets = [(mask, index, 0) for index, mask in enumerate(pairs)] + [(0, stay, 0)]
    targets += [(mask ^ core_bit, swap, index * rows) for index, mask in enumerate(pairs + [0])]
    targets += [(mask, swap + 1 + index, 0) for index, mask in enumerate(singles)]
    tiles = [(stay, rows), (swap, swap_rows), (swap + 1, rows), (swap + 2, rows)]
    constrain = lambda value: pltpu.with_memory_space_constraint(value, pltpu.HBM)
    shaped = lambda count: jax.ShapeDtypeStruct((count, LANES), jnp.float32)
    hbm = pl.BlockSpec(memory_space=pltpu.HBM)
    vmem = pl.BlockSpec(memory_space=pltpu.VMEM)
    sent = pl.pallas_call(
        lambda *refs: transform_kernel(info, targets, tiles, *refs),
        in_specs=[hbm] * 3,
        out_specs=[vmem] * len(all_rows),
        out_shape=[shaped(count) for count in all_rows],
        scratch_shapes=[
            pltpu.VMEM((vectors, LANES), jnp.float32),
            pltpu.VMEM(table.shape[1:], jnp.bfloat16),
            pltpu.VMEM(phase.shape, jnp.float32),
            pltpu.VMEM((chunks // 2, RADIX, 2 * LANES, 2 * LANES), jnp.bfloat16),
            pltpu.VMEM((chunks // 2, RADIX, 2 * LANES, 2 * LANES), jnp.bfloat16),
            pltpu.SemaphoreType.DMA((chunks + 1 + n_devices // 2,)),
        ],
        compiler_params=pltpu.CompilerParams(vmem_limit_bytes=VMEM_LIMIT),
        name="transform",
    )(constrain(x), constrain(jnp.asarray(table)), constrain(jnp.asarray(phase)))
    swapped = exchange(sent[swap], core_bit)
    arrived_singles = []
    for index, mask in enumerate(singles):
        arrived_singles.append(exchange(sent[swap + 1 + index], mask))

    def join(first, count, extra, stamps):
        n_extra = len(extra)
        return pl.pallas_call(
            lambda *refs: join_kernel(rows, first, stamps, count, *refs),
            in_specs=[vmem] * (1 + n_extra + count),
            out_specs=[vmem] * count,
            out_shape=[shaped(size) for size in pair_rows[first : first + count]],
            input_output_aliases={1 + n_extra + i: i for i in range(count)},
            compiler_params=pltpu.CompilerParams(vmem_limit_bytes=VMEM_LIMIT),
            name="join",
        )(swapped, *extra, *sent[first : first + count])

    joined = join(0, len(far), [], [])
    stamps = [(0, swap_rows), (1, rows), (2, rows), (3, rows)]
    joined += join(len(far), len(near), [sent[stay]] + arrived_singles[:2], stamps)
    arrived_pairs = []
    for index, mask in enumerate(pairs):
        arrived_pairs.append(exchange(joined[index], mask))
    arrivals = arrived_pairs + [sent[stay], swapped] + arrived_singles
    sources = []
    for index, mask in enumerate(pairs):
        sources += [(mask, index, 0), (mask ^ core_bit, index, rows)]
    sources += [(0, stay, 0), (core_bit, swap, n_pairs * rows)]
    sources += [(mask, swap + 1 + index, 0) for index, mask in enumerate(singles)]
    sums = tiles + [(len(far) + index, 2 * rows) for index in range(len(near))]
    placed, checks = pl.pallas_call(
        lambda *refs: place_kernel(place_info, sources, sums, *refs),
        in_specs=[vmem] * (1 + len(arrivals)),
        out_specs=[hbm, pl.BlockSpec(memory_space=pltpu.SMEM)],
        out_shape=[
            jax.ShapeDtypeStruct((vectors, LANES), jnp.float32),
            jax.ShapeDtypeStruct((3,), jnp.float32),
        ],
        scratch_shapes=[
            pltpu.VMEM((n_devices * slot_rows, LANES), jnp.float32),
            pltpu.VMEM((vectors, LANES), jnp.float32),
            pltpu.SemaphoreType.DMA((groups,)),
        ],
        compiler_params=pltpu.CompilerParams(vmem_limit_bytes=VMEM_LIMIT),
        name="place",
    )(jnp.asarray(order), *arrivals)
    placed = placed.reshape(vectors // 2, 2, LANES).transpose(1, 0, 2).reshape(2, amp_dev)
    return placed, checks


def solution(mesh):
    return jax.shard_map(
        per_device,
        mesh=mesh,
        in_specs=(P(None, ("outer", "inner")),),
        out_specs=(P(None, ("outer", "inner")), P()),
        check_vma=False,
    )
```

```python
import math

import jax
import jax.numpy as jnp
import ml_dtypes
import numpy as np
from jax import lax
from jax.experimental import pallas as pl
from jax.experimental.pallas import tpu as pltpu
from jax.sharding import PartitionSpec as P


WINDOW = 9
LANES = 128
RADIX = 2**WINDOW // LANES
AXES = ("outer", "inner")
VMEM_LIMIT = 16 * 2**20
SUB = 16
LEADS = 2
START_ORDER = (7, 0, 2, 3, 4, 5, 8, 9, 10, 11, 12, 13, 1, 14, 6)


def flip(value, count):
    result = 0
    for bit_pos in range(count):
        result |= (value >> bit_pos & 1) << count - 1 - bit_pos
    return result


def split_halves(table):
    high = table.astype(ml_dtypes.bfloat16)
    low = (table - high.astype(np.float64)).astype(ml_dtypes.bfloat16)
    return high, low


def transform_tables(n_devices):
    columns = 2**WINDOW
    freq = np.arange(LANES) * RADIX
    sample = np.arange(LANES)
    tables = []
    for residue in range(RADIX):
        angles = (freq + residue)[:, None] * sample[None, :] % columns * (2 * np.pi / columns)
        cosine = np.cos(angles) / math.sqrt(columns)
        sine = np.sin(angles) / math.sqrt(columns)
        rows = np.stack([np.concatenate([cosine, -sine], 1), np.concatenate([sine, cosine], 1)], 1)
        tables.append(rows.reshape(n_devices // 2, 2, 8, 2 * LANES))
    high, low = split_halves(np.stack(tables))
    both = np.concatenate([high, low], 0).transpose(1, 0, 2, 3, 4)
    both = np.stack([both, both[:, :, ::-1]])
    return both.reshape(2, n_devices // 2, 2 * RADIX, 16, 2 * LANES)


def phase_tables(chunks, n_devices, angle_scale):
    turn = np.array([flip(row, LANES.bit_length() - 1) for row in range(LANES)])
    angles = turn * float(chunks * n_devices) * angle_scale
    table = np.zeros((2, LANES, LANES))
    table[0, :, 1] = np.cos(angles)
    table[1, :, 1] = np.sin(angles)
    return table.astype(np.float32)


def plan(n_outer, n_inner):
    core_bit, far_bit = n_inner, n_inner // 2
    chip_masks = [mask for mask in range(1, n_outer * n_inner) if not mask & core_bit]
    blocks = sorted(chip_masks, key=lambda mask: (not mask & far_bit, mask.bit_count()))
    ordered = [blocks[place] for place in START_ORDER if place < len(blocks)]
    leads, rest = ordered[:LEADS], ordered[LEADS:]
    far = [mask for mask in rest if mask & far_bit]
    near = [mask for mask in rest if not mask & far_bit]
    return leads, far, near, [(far + near).index(mask) for mask in rest]


def fits(amp_dev, n_outer, n_inner):
    n_devices = n_outer * n_inner
    chunks = amp_dev // 2**WINDOW // LANES
    same_tile = 2**WINDOW // n_devices // RADIX * 2 == 8
    return chunks * n_devices == LANES and same_tile and n_inner > 1 and n_outer > 1


def halves(values):
    high = values.astype(jnp.bfloat16)
    low = (values - high.astype(jnp.float32)).astype(jnp.bfloat16)
    return high, low


def dot_rows(left, right):
    return lax.dot_general(
        left, right, (((1,), (1,)), ((), ())), preferred_element_type=jnp.float32
    )


def transform_kernel(info, targets, tiles, x_hbm, table_hbm, phase_hbm, *refs):
    n_devices, chunks, angle_scale, device_id = info()
    outs, (x_ref, table_ref, phase_ref, high_ref, low_ref, sems) = refs[:-6], refs[-6:]
    chunk_rows = RADIX * 8
    x_rows = x_ref.shape[0] // chunks
    dev_bits = n_devices.bit_length() - 1
    chunk_bits = chunks.bit_length() - 1

    def load(source, target, index):
        return pltpu.make_async_copy(source, target, sems.at[index])

    loads = []
    for chunk in range(chunks):
        rows = pl.ds(chunk * x_rows, x_rows)
        loads.append(load(x_hbm.at[rows], x_ref.at[rows], chunk))
    phase_load = load(phase_hbm, phase_ref, chunks)
    table_loads = [
        load(
            table_hbm.at[device_id & 1, (device_id >> 1) ^ block],
            table_ref.at[block],
            chunks + 1 + block,
        )
        for block in range(n_devices // 2)
    ]
    for copy in loads[:1] + [phase_load] + loads[1:] + table_loads:
        copy.start()

    base = jnp.int32(0)
    for bit in range(dev_bits):
        base += (device_id >> bit & 1) << (dev_bits - 1 - bit)
    square_sum = real_sum = imag_sum = jnp.zeros((8, LANES), jnp.float32)
    fold = lambda value: value.reshape(SUB // 8, 8, LANES).sum(0)
    for half in range(chunks // 2):
        for chunk in (2 * half, 2 * half + 1):
            loads[chunk].wait()
            if chunk == 0:
                phase_load.wait()
            turn_re = turn_im = jnp.zeros((8, LANES), jnp.float32)
            for sub in range(LANES // SUB):
                start = chunk * x_rows + sub * SUB * 2 * RADIX
                parts = [
                    [x_ref[pl.ds(start + 2 * j + s, SUB, stride=2 * RADIX), :] for s in range(2)]
                    for j in range(RADIX)
                ]
                square_sum += fold(sum(p * p for pair in parts for p in pair))
                cosine = phase_ref[0, sub * SUB : (sub + 1) * SUB]
                sine = phase_ref[1, sub * SUB : (sub + 1) * SUB]
                first_re, first_im = parts[0]
                turn_re += fold(first_re * cosine + first_im * sine)
                turn_im += fold(first_im * cosine - first_re * sine)
                (r0, i0), (r1, i1), (r2, i2), (r3, i3) = parts
                ar, ai, br, bi = r0 + r2, i0 + i2, r0 - r2, i0 - i2
                cr, ci, dr, di = r1 + r3, i1 + i3, r1 - r3, i1 - i3
                folded = [
                    (ar + cr, ai + ci),
                    (br - di, bi + dr),
                    (ar - cr, ai - ci),
                    (br + di, bi - dr),
                ]
                row = (chunk % 2) * LANES + sub * SUB
                for residue in range(RADIX):
                    for part in range(2):
                        high, low = halves(folded[residue][part])
                        where = (half, residue, pl.ds(row, SUB), pl.ds(part * LANES, LANES))
                        high_ref[where] = high
                        low_ref[where] = low
            angle = flip(chunk, chunk_bits) * n_devices * angle_scale
            cosine, sine = math.cos(angle), math.sin(angle)
            real_sum += turn_re * cosine + turn_im * sine
            imag_sum += turn_im * cosine - turn_re * sine
    for copy in table_loads:
        copy.wait()
    for half in range(chunks // 2):
        for residue in range(RADIX):
            table_high = table_ref[:, residue].reshape(2 * LANES, 2 * LANES)
            table_low = table_ref[:, RADIX + residue].reshape(2 * LANES, 2 * LANES)
            high, low = high_ref[half, residue], low_ref[half, residue]
            values = dot_rows(table_high, high) + dot_rows(table_high, low)
            values += dot_rows(table_low, high)
            for mask, out, row in targets:
                for part in range(2):
                    rows = pl.ds(row + (2 * half + part) * chunk_rows + residue * 8, 8)
                    outs[out][rows, :] = values[
                        8 * mask : 8 * mask + 8, part * LANES : (part + 1) * LANES
                    ]

    theta = jnp.full((8, LANES), base, jnp.int32).astype(jnp.float32) * angle_scale
    theta_sq = theta * theta
    cosine = 1.0 - theta_sq * (0.5 - theta_sq * (1.0 / 24.0))
    sine = theta * (1.0 - theta_sq * (1.0 / 6.0 - theta_sq * (1.0 / 120.0)))
    turned = (square_sum, real_sum * cosine + imag_sum * sine, imag_sum * cosine - real_sum * sine)
    sums = [value.sum(0, keepdims=True) for value in turned]
    tile = jnp.concatenate(sums + [jnp.zeros((5, LANES), jnp.float32)], 0)
    for out, row in tiles:
        outs[out][pl.ds(row, 8), :] = tile


def join_kernel(rows, first, stamps, n_join, swapped_ref, *refs):
    refs = (swapped_ref,) + refs
    outs = refs[len(refs) - n_join :]
    tile = None
    for operand, row in stamps:
        value = refs[operand][pl.ds(row, 8), :]
        tile = value if tile is None else tile + value
    for index, out in enumerate(outs):
        out[pl.ds(rows, rows), :] = swapped_ref[pl.ds((first + index) * rows, rows), :]
        if tile is not None:
            out[pl.ds(2 * rows, 8), :] = tile


def keep(info, sources, ins, held):
    n_devices, chunks, _, _, device_id = info()
    dev_bits = n_devices.bit_length() - 1
    slot_rows = held.shape[0] // n_devices
    turned_id = jnp.int32(0)
    for bit in range(dev_bits):
        turned_id += (device_id >> bit & 1) << (dev_bits - 1 - bit)
    rows = chunks * RADIX * 8
    for mask, array, offset in sources:
        slot = turned_id ^ flip(mask, dev_bits)
        target = pl.ds(pl.multiple_of(slot * slot_rows, 8), rows)
        held[target, :] = ins[array][pl.ds(offset, rows), :]


def stash_kernel(info, sources, tiles, *refs):
    ins, (held, sum_ref) = refs[:-2], refs[-2:]
    keep(info, sources, ins, held)
    tile = jnp.zeros((8, LANES), jnp.float32)
    for array, offset in tiles:
        tile = tile + ins[array][pl.ds(offset, 8), :]
    sum_ref[...] = tile


def place_kernel(info, sources, order_ref, held_ref, sum_ref, *refs):
    n_devices, chunks, groups, total_len, _ = info()
    ins = refs[:-5]
    out_hbm, checks_ref, held, out_ref, sems = refs[-5:]
    chunk_bits = chunks.bit_length() - 1
    slot_rows = held.shape[0] // n_devices
    keep(info, sources, ins, held)
    tile = sum_ref[...]
    sums = tile.sum(1, keepdims=True)
    mean_square = jnp.broadcast_to(sums[0:1], (8, LANES)) * (1.0 / total_len)
    shifted = mean_square + 1e-06
    factor = lax.rsqrt(shifted)
    factor = factor * (1.5 - 0.5 * shifted * factor * factor)
    columns = 2**WINDOW
    scaled = factor * math.sqrt(columns / total_len)
    checks_ref[0] = mean_square[0, 0]
    checks_ref[1] = (jnp.broadcast_to(sums[1:2], (8, LANES)) * scaled)[0, 0]
    checks_ref[2] = (jnp.broadcast_to(sums[2:3], (8, LANES)) * scaled)[0, 0]

    factor = jnp.broadcast_to(factor[0:1], (LANES, LANES))
    order = order_ref[...]
    copies = []
    for group in range(groups):
        for residue in range(RADIX):
            for part in range(2):
                pieces = []
                for low in range(chunks):
                    tile_row = (flip(low, chunk_bits) * RADIX + residue) * 8 + 2 * group + part
                    pieces.append(held[pl.ds(tile_row, n_devices, stride=slot_rows), :])
                high, low = halves(jnp.concatenate(pieces, 0))
                turned = dot_rows(order, jnp.concatenate([high, low], 1))
                row = (group * RADIX + residue) * 2 * LANES + part
                out_ref[pl.ds(row, LANES, stride=2), :] = turned * factor
            if residue % 2 == 1:
                size = 4 * LANES
                span = pl.ds(len(copies) * size, size)
                sem = sems.at[len(copies)]
                copies.append(pltpu.make_async_copy(out_ref.at[span], out_hbm.at[span], sem))
                copies[-1].start()
    for copy in copies:
        copy.wait()


def reverse_index(values, count):
    result = jnp.zeros_like(values)
    for bit_pos in range(count):
        result = result | (values >> bit_pos & 1) << count - 1 - bit_pos
    return result


def reversal_table(size, count):
    indices = jnp.arange(size, dtype=jnp.int32)
    return (reverse_index(indices, count)[:, None] == indices[None, :]).astype(jnp.float32)


def check_terms(current, positions, angle_scale):
    angles = positions.astype(jnp.float32) * angle_scale
    cosine = jnp.cos(angles)
    sine = jnp.sin(angles)
    squares = jnp.sum(current * current)
    phase_real = jnp.sum(current[0] * cosine + current[1] * sine)
    phase_imag = jnp.sum(current[1] * cosine - current[0] * sine)
    return (squares, phase_real, phase_imag)


def general_device(amplitudes):
    amp_dev = amplitudes.shape[1]
    n_outer = lax.axis_size("outer")
    n_inner = lax.axis_size("inner")
    outer_bits = n_outer.bit_length() - 1
    inner_bits = n_inner.bit_length() - 1
    global_bits = outer_bits + inner_bits
    local_bits = amp_dev.bit_length() - 1
    n_devices = n_outer * n_inner
    high_count = amp_dev // n_devices
    total_len = amp_dev * n_devices
    columns = 2**WINDOW
    rows_count = amp_dev // columns
    column_ids = jnp.arange(columns, dtype=jnp.int32)
    reversed_ids = reverse_index(column_ids, WINDOW)
    products = column_ids[:, None] * reversed_ids[None, :] % columns
    angles = products.astype(jnp.float32) * (2.0 * math.pi / columns)
    real_part = jnp.cos(angles) / math.sqrt(columns)
    imag_part = jnp.sin(angles) / math.sqrt(columns)
    table = jnp.concatenate(
        [jnp.concatenate([real_part, imag_part], 1), jnp.concatenate([-imag_part, real_part], 1)], 0
    )
    stacked = jnp.concatenate(
        [amplitudes[0].reshape(rows_count, columns), amplitudes[1].reshape(rows_count, columns)], 1
    )
    result = jnp.dot(
        stacked, table, precision=lax.Precision.HIGHEST, preferred_element_type=jnp.float32
    )
    windowed = jnp.stack([result[:, :columns].reshape(-1), result[:, columns:].reshape(-1)])
    device_id = lax.axis_index("outer") * n_inner + lax.axis_index("inner")
    angle_scale = 2.0 * math.pi / total_len
    local_ids = jnp.arange(amp_dev, dtype=jnp.int32)
    positions = reverse_index(device_id * amp_dev + local_ids, local_bits + global_bits)
    totals = lax.psum(check_terms(windowed, positions, angle_scale), ("outer", "inner"))
    device_table = reversal_table(n_devices, global_bits)
    high_table = reversal_table(high_count, local_bits - global_bits)
    grid = windowed.reshape(2, high_count, n_devices)
    ordered = jnp.einsum("pm,shm->sph", device_table, grid, precision=lax.Precision.HIGHEST)
    blocks = ordered.reshape(2, n_outer, n_inner, high_count)
    blocks = lax.all_to_all(
        lax.all_to_all(blocks, "outer", split_axis=1, concat_axis=1, tiled=True),
        "inner",
        split_axis=2,
        concat_axis=2,
        tiled=True,
    )
    received = blocks.reshape(2, n_devices, high_count)
    turned_high = jnp.einsum("qh,sdh->sdq", high_table, received, precision=lax.Precision.HIGHEST)
    placed = jnp.einsum("ed,sdq->sqe", device_table, turned_high, precision=lax.Precision.HIGHEST)
    reversed_field = placed.reshape(2, amp_dev)
    mean_square = totals[0] / total_len
    factor = lax.rsqrt(mean_square + 1e-06)
    scaled = factor / math.sqrt(total_len)
    checks = jnp.stack([mean_square, totals[1] * scaled, totals[2] * scaled])
    return (reversed_field * factor, checks)


def per_device(amplitudes):
    amp_dev = amplitudes.shape[1]
    n_devices = lax.axis_size("outer") * lax.axis_size("inner")
    n_inner = lax.axis_size("inner")
    total_len = amp_dev * n_devices
    columns = 2**WINDOW
    rows_count = amp_dev // columns
    chunks = rows_count // LANES
    groups = columns // n_devices // RADIX
    if not fits(amp_dev, lax.axis_size("outer"), n_inner):
        return general_device(amplitudes)
    vectors = 2 * amp_dev // LANES
    slot_rows = chunks * RADIX * 8 + 8
    x = amplitudes.reshape(2, vectors // 2, LANES).transpose(1, 0, 2).reshape(vectors, LANES)
    angle_scale = 2.0 * math.pi / total_len
    table = transform_tables(n_devices)
    phase = phase_tables(chunks, n_devices, angle_scale)
    turn = np.array([flip(lane, LANES.bit_length() - 1) for lane in range(LANES)])
    order = (turn[:, None] == np.arange(LANES)[None, :]).astype(np.float32)
    order = np.concatenate([order, order], 1).astype(ml_dtypes.bfloat16)

    rows = chunks * RADIX * 8
    core_bit = n_inner
    direct, far, near, _ = plan(lax.axis_size("outer"), n_inner)
    pairs = far + near
    n_pairs = len(pairs)
    n_far = len(far)

    def info():
        device_id = lax.axis_index("outer") * n_inner + lax.axis_index("inner")
        return n_devices, chunks, angle_scale, device_id

    def place_info():
        return n_devices, chunks, groups, total_len, info()[3]

    def exchange(values, mask):
        pairs_of = [(source, source ^ mask) for source in range(n_devices)]
        return lax.ppermute(values, AXES, pairs_of)

    singles = [mask ^ core for mask in direct for core in (0, core_bit)]
    swap_rows = (n_pairs + 1) * rows
    pair_rows = [2 * rows] * len(far) + [2 * rows + 8] * len(near)
    single_rows = [rows + 8] * 2 + [rows] * (len(singles) - 2)
    all_rows = pair_rows + [rows + 8, swap_rows + 8] + single_rows
    stay, swap = n_pairs, n_pairs + 1
    targets = [(mask, index, 0) for index, mask in enumerate(pairs)] + [(0, stay, 0)]
    targets += [(mask ^ core_bit, swap, index * rows) for index, mask in enumerate(pairs + [0])]
    targets += [(mask, swap + 1 + index, 0) for index, mask in enumerate(singles)]
    tiles = [(stay, rows), (swap, swap_rows), (swap + 1, rows), (swap + 2, rows)]
    constrain = lambda value: pltpu.with_memory_space_constraint(value, pltpu.HBM)
    shaped = lambda count: jax.ShapeDtypeStruct((count, LANES), jnp.float32)
    hbm = pl.BlockSpec(memory_space=pltpu.HBM)
    vmem = pl.BlockSpec(memory_space=pltpu.VMEM)
    sent = pl.pallas_call(
        lambda *refs: transform_kernel(info, targets, tiles, *refs),
        in_specs=[hbm] * 3,
        out_specs=[vmem] * len(all_rows),
        out_shape=[shaped(count) for count in all_rows],
        scratch_shapes=[
            pltpu.VMEM((vectors, LANES), jnp.float32),
            pltpu.VMEM(table.shape[1:], jnp.bfloat16),
            pltpu.VMEM(phase.shape, jnp.float32),
            pltpu.VMEM((chunks // 2, RADIX, 2 * LANES, 2 * LANES), jnp.bfloat16),
            pltpu.VMEM((chunks // 2, RADIX, 2 * LANES, 2 * LANES), jnp.bfloat16),
            pltpu.SemaphoreType.DMA((chunks + 1 + n_devices // 2,)),
        ],
        compiler_params=pltpu.CompilerParams(vmem_limit_bytes=VMEM_LIMIT),
        name="transform",
    )(constrain(x), constrain(jnp.asarray(table)), constrain(jnp.asarray(phase)))
    swapped = exchange(sent[swap], core_bit)
    arrived_singles = []
    for index, mask in enumerate(singles):
        arrived_singles.append(exchange(sent[swap + 1 + index], mask))

    def join(first, count, extra, stamps):
        n_extra = len(extra)
        return pl.pallas_call(
            lambda *refs: join_kernel(rows, first, stamps, count, *refs),
            in_specs=[vmem] * (1 + n_extra + count),
            out_specs=[vmem] * count,
            out_shape=[shaped(size) for size in pair_rows[first : first + count]],
            input_output_aliases={1 + n_extra + i: i for i in range(count)},
            compiler_params=pltpu.CompilerParams(vmem_limit_bytes=VMEM_LIMIT),
            name="join",
        )(swapped, *extra, *sent[first : first + count])

    joined = join(0, len(far), [], [])
    stamps = [(0, swap_rows), (1, rows), (2, rows), (3, rows)]
    joined += join(len(far), len(near), [sent[stay]] + arrived_singles[:2], stamps)
    arrived_pairs = []
    for index, mask in enumerate(pairs):
        arrived_pairs.append(exchange(joined[index], mask))
    arrivals = arrived_pairs + [sent[stay], swapped] + arrived_singles
    sources = []
    for index, mask in enumerate(pairs):
        sources += [(mask, index, 0), (mask ^ core_bit, index, rows)]
    sources += [(0, stay, 0), (core_bit, swap, n_pairs * rows)]
    sources += [(mask, swap + 1 + index, 0) for index, mask in enumerate(singles)]
    sums = tiles + [(len(far) + index, 2 * rows) for index in range(len(near))]
    params = pltpu.CompilerParams(vmem_limit_bytes=VMEM_LIMIT)
    held_rows = n_devices * slot_rows
    n_late = 2
    late = range(n_far - n_late, n_far)
    late_sources = [(mask, index - late[0], row) for mask, index, row in sources if index in late]
    early_sources = [source for source in sources if source[1] not in late]
    early = [index for index in range(len(arrivals)) if index not in late]
    renamed = lambda index: early.index(index)
    early_sources = [(mask, renamed(index), row) for mask, index, row in early_sources]
    sums = [(renamed(index), row) for index, row in sums]
    held, total = pl.pallas_call(
        lambda *refs: stash_kernel(place_info, early_sources, sums, *refs),
        in_specs=[vmem] * len(early),
        out_specs=[vmem, vmem],
        out_shape=[shaped(held_rows), shaped(8)],
        compiler_params=params,
        name="stash",
    )(*[arrivals[index] for index in early])
    placed, checks, _ = pl.pallas_call(
        lambda *refs: place_kernel(place_info, late_sources, *refs),
        in_specs=[vmem] * (3 + n_late),
        out_specs=[hbm, pl.BlockSpec(memory_space=pltpu.SMEM), vmem],
        out_shape=[
            jax.ShapeDtypeStruct((vectors, LANES), jnp.float32),
            jax.ShapeDtypeStruct((3,), jnp.float32),
            shaped(held_rows),
        ],
        input_output_aliases={1: 2},
        scratch_shapes=[
            pltpu.VMEM((vectors, LANES), jnp.float32),
            pltpu.SemaphoreType.DMA((2 * groups,)),
        ],
        compiler_params=params,
        name="place",
    )(jnp.asarray(order), held, total, *[arrivals[index] for index in late])
    placed = placed.reshape(vectors // 2, 2, LANES).transpose(1, 0, 2).reshape(2, amp_dev)
    return placed, checks


def solution(mesh):
    return jax.shard_map(
        per_device,
        mesh=mesh,
        in_specs=(P(None, ("outer", "inner")),),
        out_specs=(P(None, ("outer", "inner")), P()),
        check_vma=False,
    )
```

```python
import math

import jax
import jax.numpy as jnp
import ml_dtypes
import numpy as np
from jax import lax
from jax.experimental import pallas as pl
from jax.experimental.pallas import tpu as pltpu
from jax.sharding import PartitionSpec as P


WINDOW = 9
LANES = 128
RADIX = 2**WINDOW // LANES
AXES = ("outer", "inner")
VMEM_LIMIT = 16 * 2**20
SUB = 16
LEADS = 2
START_ORDER = (7, 0, 2, 3, 4, 5, 8, 9, 10, 11, 12, 13, 1, 14, 6)


def flip(value, count):
    result = 0
    for bit_pos in range(count):
        result |= (value >> bit_pos & 1) << count - 1 - bit_pos
    return result


def split_halves(table):
    high = table.astype(ml_dtypes.bfloat16)
    low = (table - high.astype(np.float64)).astype(ml_dtypes.bfloat16)
    return high, low


def transform_tables(n_devices):
    columns = 2**WINDOW
    freq = np.arange(LANES) * RADIX
    sample = np.arange(LANES)
    tables = []
    for residue in range(RADIX):
        angles = (freq + residue)[:, None] * sample[None, :] % columns * (2 * np.pi / columns)
        cosine = np.cos(angles) / math.sqrt(columns)
        sine = np.sin(angles) / math.sqrt(columns)
        rows = np.stack([np.concatenate([cosine, -sine], 1), np.concatenate([sine, cosine], 1)], 1)
        tables.append(rows.reshape(n_devices // 2, 2, 8, 2 * LANES))
    high, low = split_halves(np.stack(tables))
    both = np.concatenate([high, low], 0).transpose(1, 0, 2, 3, 4)
    both = np.stack([both, both[:, :, ::-1]])
    return both.reshape(2, n_devices // 2, 2 * RADIX, 16, 2 * LANES)


def phase_tables(chunks, n_devices, angle_scale):
    turn = np.array([flip(row, LANES.bit_length() - 1) for row in range(LANES)])
    angles = turn * float(chunks * n_devices) * angle_scale
    table = np.zeros((2, LANES, LANES))
    table[0, :, 1] = np.cos(angles)
    table[1, :, 1] = np.sin(angles)
    return table.astype(np.float32)


def plan(n_outer, n_inner):
    core_bit, far_bit = n_inner, n_inner // 2
    chip_masks = [mask for mask in range(1, n_outer * n_inner) if not mask & core_bit]
    blocks = sorted(chip_masks, key=lambda mask: (not mask & far_bit, mask.bit_count()))
    ordered = [blocks[place] for place in START_ORDER if place < len(blocks)]
    leads, rest = ordered[:LEADS], ordered[LEADS:]
    far = [mask for mask in rest if mask & far_bit]
    near = [mask for mask in rest if not mask & far_bit]
    return leads, far, near, [(far + near).index(mask) for mask in rest]


def fits(amp_dev, n_outer, n_inner):
    n_devices = n_outer * n_inner
    chunks = amp_dev // 2**WINDOW // LANES
    same_tile = 2**WINDOW // n_devices // RADIX * 2 == 8
    return chunks * n_devices == LANES and same_tile and n_inner > 1 and n_outer > 1


def halves(values):
    high = values.astype(jnp.bfloat16)
    low = (values - high.astype(jnp.float32)).astype(jnp.bfloat16)
    return high, low


def dot_rows(left, right):
    return lax.dot_general(
        left, right, (((1,), (1,)), ((), ())), preferred_element_type=jnp.float32
    )


def transform_kernel(info, targets, tiles, x_hbm, table_hbm, phase_hbm, *refs):
    n_devices, chunks, angle_scale, device_id = info()
    outs, (x_ref, table_ref, phase_ref, high_ref, low_ref, sems) = refs[:-6], refs[-6:]
    chunk_rows = RADIX * 8
    x_rows = x_ref.shape[0] // chunks
    dev_bits = n_devices.bit_length() - 1
    chunk_bits = chunks.bit_length() - 1

    def load(source, target, index):
        return pltpu.make_async_copy(source, target, sems.at[index])

    loads = []
    for chunk in range(chunks):
        rows = pl.ds(chunk * x_rows, x_rows)
        loads.append(load(x_hbm.at[rows], x_ref.at[rows], chunk))
    phase_load = load(phase_hbm, phase_ref, chunks)
    table_loads = [
        load(
            table_hbm.at[device_id & 1, (device_id >> 1) ^ block],
            table_ref.at[block],
            chunks + 1 + block,
        )
        for block in range(n_devices // 2)
    ]
    for copy in loads[:1] + [phase_load] + loads[1:] + table_loads:
        copy.start()

    base = jnp.int32(0)
    for bit in range(dev_bits):
        base += (device_id >> bit & 1) << (dev_bits - 1 - bit)
    square_sum = real_sum = imag_sum = jnp.zeros((8, LANES), jnp.float32)
    fold = lambda value: value.reshape(SUB // 8, 8, LANES).sum(0)
    for half in range(chunks // 2):
        for chunk in (2 * half, 2 * half + 1):
            loads[chunk].wait()
            if chunk == 0:
                phase_load.wait()
            turn_re = turn_im = jnp.zeros((8, LANES), jnp.float32)
            for sub in range(LANES // SUB):
                start = chunk * x_rows + sub * SUB * 2 * RADIX
                parts = [
                    [x_ref[pl.ds(start + 2 * j + s, SUB, stride=2 * RADIX), :] for s in range(2)]
                    for j in range(RADIX)
                ]
                square_sum += fold(sum(p * p for pair in parts for p in pair))
                cosine = phase_ref[0, sub * SUB : (sub + 1) * SUB]
                sine = phase_ref[1, sub * SUB : (sub + 1) * SUB]
                first_re, first_im = parts[0]
                turn_re += fold(first_re * cosine + first_im * sine)
                turn_im += fold(first_im * cosine - first_re * sine)
                (r0, i0), (r1, i1), (r2, i2), (r3, i3) = parts
                ar, ai, br, bi = r0 + r2, i0 + i2, r0 - r2, i0 - i2
                cr, ci, dr, di = r1 + r3, i1 + i3, r1 - r3, i1 - i3
                folded = [
                    (ar + cr, ai + ci),
                    (br - di, bi + dr),
                    (ar - cr, ai - ci),
                    (br + di, bi - dr),
                ]
                row = (chunk % 2) * LANES + sub * SUB
                for residue in range(RADIX):
                    for part in range(2):
                        high, low = halves(folded[residue][part])
                        where = (half, residue, pl.ds(row, SUB), pl.ds(part * LANES, LANES))
                        high_ref[where] = high
                        low_ref[where] = low
            angle = flip(chunk, chunk_bits) * n_devices * angle_scale
            cosine, sine = math.cos(angle), math.sin(angle)
            real_sum += turn_re * cosine + turn_im * sine
            imag_sum += turn_im * cosine - turn_re * sine
    for copy in table_loads:
        copy.wait()
    for half in range(chunks // 2):
        for residue in range(RADIX):
            table_high = table_ref[:, residue].reshape(2 * LANES, 2 * LANES)
            table_low = table_ref[:, RADIX + residue].reshape(2 * LANES, 2 * LANES)
            high, low = high_ref[half, residue], low_ref[half, residue]
            values = dot_rows(table_high, high) + dot_rows(table_high, low)
            values += dot_rows(table_low, high)
            for mask, out, row in targets:
                for part in range(2):
                    rows = pl.ds(row + (2 * half + part) * chunk_rows + residue * 8, 8)
                    outs[out][rows, :] = values[
                        8 * mask : 8 * mask + 8, part * LANES : (part + 1) * LANES
                    ]

    theta = jnp.full((8, LANES), base, jnp.int32).astype(jnp.float32) * angle_scale
    theta_sq = theta * theta
    cosine = 1.0 - theta_sq * (0.5 - theta_sq * (1.0 / 24.0))
    sine = theta * (1.0 - theta_sq * (1.0 / 6.0 - theta_sq * (1.0 / 120.0)))
    turned = (square_sum, real_sum * cosine + imag_sum * sine, imag_sum * cosine - real_sum * sine)
    sums = [value.sum(0, keepdims=True) for value in turned]
    tile = jnp.concatenate(sums + [jnp.zeros((5, LANES), jnp.float32)], 0)
    for out, row in tiles:
        outs[out][pl.ds(row, 8), :] = tile


def join_kernel(rows, first, stamps, n_join, swapped_ref, *refs):
    refs = (swapped_ref,) + refs
    outs = refs[len(refs) - n_join :]
    tile = None
    for operand, row in stamps:
        value = refs[operand][pl.ds(row, 8), :]
        tile = value if tile is None else tile + value
    for index, out in enumerate(outs):
        out[pl.ds(rows, rows), :] = swapped_ref[pl.ds((first + index) * rows, rows), :]
        if tile is not None:
            out[pl.ds(2 * rows, 8), :] = tile


def keep(info, sources, ins, held):
    n_devices, chunks, _, _, device_id = info()
    dev_bits = n_devices.bit_length() - 1
    slot_rows = held.shape[0] // n_devices
    turned_id = jnp.int32(0)
    for bit in range(dev_bits):
        turned_id += (device_id >> bit & 1) << (dev_bits - 1 - bit)
    rows = chunks * RADIX * 8
    for mask, array, offset in sources:
        slot = turned_id ^ flip(mask, dev_bits)
        target = pl.ds(pl.multiple_of(slot * slot_rows, 8), rows)
        held[target, :] = ins[array][pl.ds(offset, rows), :]


def stash_kernel(info, sources, tiles, *refs):
    ins, (held, sum_ref) = refs[:-2], refs[-2:]
    keep(info, sources, ins, held)
    tile = jnp.zeros((8, LANES), jnp.float32)
    for array, offset in tiles:
        tile = tile + ins[array][pl.ds(offset, 8), :]
    sum_ref[...] = tile


def place_kernel(info, sources, order_ref, held_ref, sum_ref, *refs):
    n_devices, chunks, groups, total_len, _ = info()
    ins = refs[:-5]
    out_hbm, checks_ref, held, out_ref, sems = refs[-5:]
    chunk_bits = chunks.bit_length() - 1
    slot_rows = held.shape[0] // n_devices
    keep(info, sources, ins, held)
    tile = sum_ref[...]
    sums = tile.sum(1, keepdims=True)
    mean_square = jnp.broadcast_to(sums[0:1], (8, LANES)) * (1.0 / total_len)
    shifted = mean_square + 1e-06
    factor = lax.rsqrt(shifted)
    factor = factor * (1.5 - 0.5 * shifted * factor * factor)
    columns = 2**WINDOW
    scaled = factor * math.sqrt(columns / total_len)
    checks_ref[0] = mean_square[0, 0]
    checks_ref[1] = (jnp.broadcast_to(sums[1:2], (8, LANES)) * scaled)[0, 0]
    checks_ref[2] = (jnp.broadcast_to(sums[2:3], (8, LANES)) * scaled)[0, 0]

    factor = jnp.broadcast_to(factor[0:1], (LANES, LANES))
    order = order_ref[...]
    copies = []
    for group in range(groups):
        for residue in range(RADIX):
            for part in range(2):
                pieces = []
                for low in range(chunks):
                    tile_row = (flip(low, chunk_bits) * RADIX + residue) * 8 + 2 * group + part
                    pieces.append(held[pl.ds(tile_row, n_devices, stride=slot_rows), :])
                high, low = halves(jnp.concatenate(pieces, 0))
                turned = dot_rows(order, jnp.concatenate([high, low], 1))
                row = (group * RADIX + residue) * 2 * LANES + part
                out_ref[pl.ds(row, LANES, stride=2), :] = turned * factor
            size = 2 * LANES
            span = pl.ds(len(copies) * size, size)
            sem = sems.at[len(copies)]
            copies.append(pltpu.make_async_copy(out_ref.at[span], out_hbm.at[span], sem))
            copies[-1].start()
    for copy in copies:
        copy.wait()


def reverse_index(values, count):
    result = jnp.zeros_like(values)
    for bit_pos in range(count):
        result = result | (values >> bit_pos & 1) << count - 1 - bit_pos
    return result


def reversal_table(size, count):
    indices = jnp.arange(size, dtype=jnp.int32)
    return (reverse_index(indices, count)[:, None] == indices[None, :]).astype(jnp.float32)


def check_terms(current, positions, angle_scale):
    angles = positions.astype(jnp.float32) * angle_scale
    cosine = jnp.cos(angles)
    sine = jnp.sin(angles)
    squares = jnp.sum(current * current)
    phase_real = jnp.sum(current[0] * cosine + current[1] * sine)
    phase_imag = jnp.sum(current[1] * cosine - current[0] * sine)
    return (squares, phase_real, phase_imag)


def general_device(amplitudes):
    amp_dev = amplitudes.shape[1]
    n_outer = lax.axis_size("outer")
    n_inner = lax.axis_size("inner")
    outer_bits = n_outer.bit_length() - 1
    inner_bits = n_inner.bit_length() - 1
    global_bits = outer_bits + inner_bits
    local_bits = amp_dev.bit_length() - 1
    n_devices = n_outer * n_inner
    high_count = amp_dev // n_devices
    total_len = amp_dev * n_devices
    columns = 2**WINDOW
    rows_count = amp_dev // columns
    column_ids = jnp.arange(columns, dtype=jnp.int32)
    reversed_ids = reverse_index(column_ids, WINDOW)
    products = column_ids[:, None] * reversed_ids[None, :] % columns
    angles = products.astype(jnp.float32) * (2.0 * math.pi / columns)
    real_part = jnp.cos(angles) / math.sqrt(columns)
    imag_part = jnp.sin(angles) / math.sqrt(columns)
    table = jnp.concatenate(
        [jnp.concatenate([real_part, imag_part], 1), jnp.concatenate([-imag_part, real_part], 1)], 0
    )
    stacked = jnp.concatenate(
        [amplitudes[0].reshape(rows_count, columns), amplitudes[1].reshape(rows_count, columns)], 1
    )
    result = jnp.dot(
        stacked, table, precision=lax.Precision.HIGHEST, preferred_element_type=jnp.float32
    )
    windowed = jnp.stack([result[:, :columns].reshape(-1), result[:, columns:].reshape(-1)])
    device_id = lax.axis_index("outer") * n_inner + lax.axis_index("inner")
    angle_scale = 2.0 * math.pi / total_len
    local_ids = jnp.arange(amp_dev, dtype=jnp.int32)
    positions = reverse_index(device_id * amp_dev + local_ids, local_bits + global_bits)
    totals = lax.psum(check_terms(windowed, positions, angle_scale), ("outer", "inner"))
    device_table = reversal_table(n_devices, global_bits)
    high_table = reversal_table(high_count, local_bits - global_bits)
    grid = windowed.reshape(2, high_count, n_devices)
    ordered = jnp.einsum("pm,shm->sph", device_table, grid, precision=lax.Precision.HIGHEST)
    blocks = ordered.reshape(2, n_outer, n_inner, high_count)
    blocks = lax.all_to_all(
        lax.all_to_all(blocks, "outer", split_axis=1, concat_axis=1, tiled=True),
        "inner",
        split_axis=2,
        concat_axis=2,
        tiled=True,
    )
    received = blocks.reshape(2, n_devices, high_count)
    turned_high = jnp.einsum("qh,sdh->sdq", high_table, received, precision=lax.Precision.HIGHEST)
    placed = jnp.einsum("ed,sdq->sqe", device_table, turned_high, precision=lax.Precision.HIGHEST)
    reversed_field = placed.reshape(2, amp_dev)
    mean_square = totals[0] / total_len
    factor = lax.rsqrt(mean_square + 1e-06)
    scaled = factor / math.sqrt(total_len)
    checks = jnp.stack([mean_square, totals[1] * scaled, totals[2] * scaled])
    return (reversed_field * factor, checks)


def per_device(amplitudes):
    amp_dev = amplitudes.shape[1]
    n_devices = lax.axis_size("outer") * lax.axis_size("inner")
    n_inner = lax.axis_size("inner")
    total_len = amp_dev * n_devices
    columns = 2**WINDOW
    rows_count = amp_dev // columns
    chunks = rows_count // LANES
    groups = columns // n_devices // RADIX
    if not fits(amp_dev, lax.axis_size("outer"), n_inner):
        return general_device(amplitudes)
    vectors = 2 * amp_dev // LANES
    slot_rows = chunks * RADIX * 8 + 8
    x = amplitudes.reshape(2, vectors // 2, LANES).transpose(1, 0, 2).reshape(vectors, LANES)
    angle_scale = 2.0 * math.pi / total_len
    table = transform_tables(n_devices)
    phase = phase_tables(chunks, n_devices, angle_scale)
    turn = np.array([flip(lane, LANES.bit_length() - 1) for lane in range(LANES)])
    order = (turn[:, None] == np.arange(LANES)[None, :]).astype(np.float32)
    order = np.concatenate([order, order], 1).astype(ml_dtypes.bfloat16)

    rows = chunks * RADIX * 8
    core_bit = n_inner
    direct, far, near, _ = plan(lax.axis_size("outer"), n_inner)
    pairs = far + near
    n_pairs = len(pairs)
    n_far = len(far)

    def info():
        device_id = lax.axis_index("outer") * n_inner + lax.axis_index("inner")
        return n_devices, chunks, angle_scale, device_id

    def place_info():
        return n_devices, chunks, groups, total_len, info()[3]

    def exchange(values, mask):
        pairs_of = [(source, source ^ mask) for source in range(n_devices)]
        return lax.ppermute(values, AXES, pairs_of)

    singles = [mask ^ core for mask in direct for core in (0, core_bit)]
    swap_rows = (n_pairs + 1) * rows
    pair_rows = [2 * rows] * len(far) + [2 * rows + 8] * len(near)
    single_rows = [rows + 8] * 2 + [rows] * (len(singles) - 2)
    all_rows = pair_rows + [rows + 8, swap_rows + 8] + single_rows
    stay, swap = n_pairs, n_pairs + 1
    targets = [(mask, index, 0) for index, mask in enumerate(pairs)] + [(0, stay, 0)]
    targets += [(mask ^ core_bit, swap, index * rows) for index, mask in enumerate(pairs + [0])]
    targets += [(mask, swap + 1 + index, 0) for index, mask in enumerate(singles)]
    tiles = [(stay, rows), (swap, swap_rows), (swap + 1, rows), (swap + 2, rows)]
    constrain = lambda value: pltpu.with_memory_space_constraint(value, pltpu.HBM)
    shaped = lambda count: jax.ShapeDtypeStruct((count, LANES), jnp.float32)
    hbm = pl.BlockSpec(memory_space=pltpu.HBM)
    vmem = pl.BlockSpec(memory_space=pltpu.VMEM)
    sent = pl.pallas_call(
        lambda *refs: transform_kernel(info, targets, tiles, *refs),
        in_specs=[hbm] * 3,
        out_specs=[vmem] * len(all_rows),
        out_shape=[shaped(count) for count in all_rows],
        scratch_shapes=[
            pltpu.VMEM((vectors, LANES), jnp.float32),
            pltpu.VMEM(table.shape[1:], jnp.bfloat16),
            pltpu.VMEM(phase.shape, jnp.float32),
            pltpu.VMEM((chunks // 2, RADIX, 2 * LANES, 2 * LANES), jnp.bfloat16),
            pltpu.VMEM((chunks // 2, RADIX, 2 * LANES, 2 * LANES), jnp.bfloat16),
            pltpu.SemaphoreType.DMA((chunks + 1 + n_devices // 2,)),
        ],
        compiler_params=pltpu.CompilerParams(vmem_limit_bytes=VMEM_LIMIT),
        name="transform",
    )(constrain(x), constrain(jnp.asarray(table)), constrain(jnp.asarray(phase)))
    swapped = exchange(sent[swap], core_bit)
    arrived_singles = []
    for index, mask in enumerate(singles):
        arrived_singles.append(exchange(sent[swap + 1 + index], mask))

    def join(first, count, extra, stamps):
        n_extra = len(extra)
        return pl.pallas_call(
            lambda *refs: join_kernel(rows, first, stamps, count, *refs),
            in_specs=[vmem] * (1 + n_extra + count),
            out_specs=[vmem] * count,
            out_shape=[shaped(size) for size in pair_rows[first : first + count]],
            input_output_aliases={1 + n_extra + i: i for i in range(count)},
            compiler_params=pltpu.CompilerParams(vmem_limit_bytes=VMEM_LIMIT),
            name="join",
        )(swapped, *extra, *sent[first : first + count])

    joined = join(0, len(far), [], [])
    stamps = [(0, swap_rows), (1, rows), (2, rows), (3, rows)]
    joined += join(len(far), len(near), [sent[stay]] + arrived_singles[:2], stamps)
    arrived_pairs = []
    for index, mask in enumerate(pairs):
        arrived_pairs.append(exchange(joined[index], mask))
    arrivals = arrived_pairs + [sent[stay], swapped] + arrived_singles
    sources = []
    for index, mask in enumerate(pairs):
        sources += [(mask, index, 0), (mask ^ core_bit, index, rows)]
    sources += [(0, stay, 0), (core_bit, swap, n_pairs * rows)]
    sources += [(mask, swap + 1 + index, 0) for index, mask in enumerate(singles)]
    sums = tiles + [(len(far) + index, 2 * rows) for index in range(len(near))]
    params = pltpu.CompilerParams(vmem_limit_bytes=VMEM_LIMIT)
    held_rows = n_devices * slot_rows
    n_late = 2
    late = range(n_far - n_late, n_far)
    late_sources = [(mask, index - late[0], row) for mask, index, row in sources if index in late]
    early_sources = [source for source in sources if source[1] not in late]
    early = [index for index in range(len(arrivals)) if index not in late]
    renamed = lambda index: early.index(index)
    early_sources = [(mask, renamed(index), row) for mask, index, row in early_sources]
    sums = [(renamed(index), row) for index, row in sums]
    held, total = pl.pallas_call(
        lambda *refs: stash_kernel(place_info, early_sources, sums, *refs),
        in_specs=[vmem] * len(early),
        out_specs=[vmem, vmem],
        out_shape=[shaped(held_rows), shaped(8)],
        compiler_params=params,
        name="stash",
    )(*[arrivals[index] for index in early])
    placed, checks, _ = pl.pallas_call(
        lambda *refs: place_kernel(place_info, late_sources, *refs),
        in_specs=[vmem] * (3 + n_late),
        out_specs=[hbm, pl.BlockSpec(memory_space=pltpu.SMEM), vmem],
        out_shape=[
            jax.ShapeDtypeStruct((vectors, LANES), jnp.float32),
            jax.ShapeDtypeStruct((3,), jnp.float32),
            shaped(held_rows),
        ],
        input_output_aliases={1: 2},
        scratch_shapes=[
            pltpu.VMEM((vectors, LANES), jnp.float32),
            pltpu.SemaphoreType.DMA((RADIX * groups,)),
        ],
        compiler_params=params,
        name="place",
    )(jnp.asarray(order), held, total, *[arrivals[index] for index in late])
    placed = placed.reshape(vectors // 2, 2, LANES).transpose(1, 0, 2).reshape(2, amp_dev)
    return placed, checks


def solution(mesh):
    return jax.shard_map(
        per_device,
        mesh=mesh,
        in_specs=(P(None, ("outer", "inner")),),
        out_specs=(P(None, ("outer", "inner")), P()),
        check_vma=False,
    )
```
